256 devices in a mesh: grp: 4 (over y), mem: 64 (over z, x, core).
Axes of the slice: x: 4, y: 4, z: 8, core: 2. Of those that a mesh axis runs over, the one named last changes fastest.
Arguments:
- values: bfloat16 [256, 64, 32, 128], P(('grp', 'mem')), may hold values from -6 to 6
- slots: int32 [256, 64, 32], P(('grp', 'mem')), may hold values from 0 to 7167
- counts: int32 [256, 64], P(('grp', 'mem')), may hold values from 0 to 32, as said below
Outputs:
- averaged: float32 [458752, 128], P('mem')
- returned: bfloat16 [256, 64, 32, 128], P(('grp', 'mem'))
The draws below stay inside these ranges and needn't reach their ends.
Inputs may be any that keep to these rules, and one draw needn't show every extreme that they name: `counts`: every device has at least one list with exactly 32 valid entries.
All inputs are finite; a program needn't handle non-finite values.
Results may differ from the reference program's by a relative error of at most 0.0024.
Values may be sent and summed in bfloat16 or wider, within the bound.
A program may use at most 64 MiB of HBM per device.

```python
import jax
import jax.numpy as jnp

BLOCK = 128
BUCKET = 7168
CAP = 32
SENDERS = 256
N_MEM = 64


def draw_counts(key, part):
    key_load, key_base, key_full = jax.random.split(jax.random.fold_in(key, 7), 3)
    owner_load = jax.random.randint(key_load, (1, N_MEM), 1, 5)
    base_count = jax.random.randint(key_base, (SENDERS, N_MEM), 0, CAP + 1)
    scaled = jnp.minimum(base_count * owner_load // 2, CAP)
    full_list = jax.random.randint(key_full, (SENDERS, 1), 0, N_MEM)
    columns = jnp.arange(N_MEM, dtype=jnp.int32)[None, :]
    return jnp.where(columns == full_list, CAP, scaled).astype(jnp.int32)


def touch_ends(result, own_key, smallest, top_value):
    longest = result.shape.index(max(result.shape))
    spots = []
    for shift in (0, 1):
        where = [jax.random.randint(jax.random.fold_in(own_key, axis), (), 0, length) for axis, length in enumerate(result.shape)]
        where[longest] = (where[longest] + shift) % result.shape[longest]
        spots.append(tuple(where))
    return result.at[spots[0]].set(smallest).at[spots[1]].set(top_value)


def level_of(own_key, dims, cuts, low, high):
    def one(dim, parts):
        draws = jax.random.uniform(jax.random.fold_in(jax.random.fold_in(own_key, 6), dim), (parts,), jnp.float32, low / len(cuts), high / len(cuts))
        return jnp.repeat(jnp.exp(draws), dims[dim] // parts).reshape((-1,) + (1,) * (len(dims) - dim - 1))

    factor_of = one(*cuts[0])
    for cut in cuts[1:]:
        factor_of = factor_of * one(*cut)
    return factor_of


def noise(own_key, shape, deviation, limit, cuts=(), kind=jnp.bfloat16):
    drawn = deviation * jax.random.normal(own_key, shape, jnp.float32)
    if cuts:
        drawn = drawn * level_of(own_key, shape, cuts, -0.22, 0.18)
    return jnp.clip(drawn, -limit, limit).astype(kind)


def setup_inputs(seed: int = 0) -> dict:
    key_list = jax.random.split(jax.random.key(seed), 4)
    return {
        "values": noise(key_list[0], (SENDERS, N_MEM, CAP, BLOCK), 1.0, 6.0, ((0, 256),)),
        "slots": touch_ends(jax.random.randint(key_list[1], (SENDERS, N_MEM, CAP), 0, BUCKET), jax.random.fold_in(key_list[1], 1), 0, BUCKET - 1).astype(jnp.int32),
        "counts": draw_counts(jax.random.fold_in(key_list[3], 71), 0),
    }


def reference(values, slots, counts):
    is_valid = jnp.arange(CAP, dtype=jnp.int32)[None, None, :] < counts[:, :, None]
    target = (jnp.arange(N_MEM, dtype=jnp.int32)[None, :, None] * BUCKET + slots).reshape(-1)
    masked = jnp.where(is_valid[..., None], values.astype(jnp.float32), jnp.float32(0.0)).reshape(-1, BLOCK)
    slot_sums = jax.ops.segment_sum(masked, target, num_segments=N_MEM * BUCKET)
    slot_count = jax.ops.segment_sum(is_valid.reshape(-1).astype(jnp.float32), target, num_segments=N_MEM * BUCKET)
    averaged = slot_sums / jnp.maximum(slot_count, jnp.float32(1.0))[:, None]
    picked = jnp.take(averaged, target, axis=0).reshape(values.shape)
    returned = jnp.where(is_valid[..., None], picked, jnp.float32(0.0)).astype(jnp.bfloat16)
    return averaged, returned
```

```python
import functools

import jax
import jax.numpy as jnp
from jax import lax
from jax.experimental import pallas as pl
from jax.experimental.pallas import tpu as pltpu
from jax.sharding import PartitionSpec as P

MESH = pl.DeviceIdType.MESH

GROUPS = 4
MEMBERS = 64
CAP = 32
BLOCK = 128
BUCKET = 7168
HALF = BUCKET // 2
PER_CHUNK = 8
CHUNKS = MEMBERS // PER_CHUNK
PAIR = 2 * PER_CHUNK
PIECE = PAIR * CAP
PIECES = MEMBERS // PAIR


def z_step(chunk):
    odd = chunk % 2
    return odd * ((chunk + 1) // 2) + (1 - odd) * ((8 - chunk // 2) % 8)


def member_at(me, chunk, place, sign):
    z, x, core = me // 8, (me // 2) % 4, me % 2
    z_to = (z + 8 + sign * z_step(chunk)) % 8
    x_to = (x + 4 + sign * (place // 2)) % 4
    core_to = (core + place) % 2
    return z_to * 8 + x_to * 2 + core_to


def lanes(shape):
    return lax.broadcasted_iota(jnp.int32, shape, len(shape) - 1)


def in_half(slot):
    return jnp.where(slot >= HALF, slot - HALF, slot)


def kernel(
    values, slots, counts, averaged_out, returned_out,
    vals, raw_slots, raw_counts, sent_slots, rows, row_slots, flat, lane_slots, wide_slots,
    sums, tally, mean, averaged, back,
    load_sem, out_sem, send_sem, own_sem, ring_sem, slot_sem, back_sem,
):
    group = lax.axis_index("grp")
    me = lax.axis_index("mem")
    up, down = (group + 1) % GROUPS, (group + GROUPS - 1) % GROUPS

    barrier = pltpu.get_barrier_semaphore()

    def greet(k, _):
        to = member_at(me, k // PER_CHUNK, k % PER_CHUNK, 1)
        pl.semaphore_signal(barrier, inc=1, device_id={"grp": group, "mem": to}, device_id_type=MESH)
        return 0

    lax.fori_loop(1, MEMBERS, greet, 0)
    for other in (up, down):
        pl.semaphore_signal(barrier, inc=1, device_id={"grp": other, "mem": me}, device_id_type=MESH)

    load_slots = pltpu.make_async_copy(slots.at[0], raw_slots, load_sem.at[0])
    load_counts = pltpu.make_async_copy(counts, raw_counts, load_sem.at[1])
    load_values = pltpu.make_async_copy(values.at[0], vals, load_sem.at[2])
    load_own = pltpu.make_async_copy(values.at[0, me], rows.at[0, 0], load_sem.at[3])
    load_slots.start()
    load_counts.start()
    load_values.start()
    load_own.start()

    load_slots.wait()
    load_counts.wait()
    square = (MEMBERS, MEMBERS)
    on_diagonal = lax.broadcasted_iota(jnp.int32, square, 0) == lanes(square)
    spread = jnp.broadcast_to(raw_counts[...], square)
    count_column = jnp.sum(jnp.where(on_diagonal, spread, 0).astype(jnp.float32), axis=1, keepdims=True)
    count_column = count_column.astype(jnp.int32)
    mine = raw_slots[...]
    tiled = jnp.concatenate([mine, mine, mine, mine], axis=1)
    is_valid = lanes(tiled.shape) % CAP < count_column
    sent_slots[...] = jnp.where(is_valid, tiled, -1).reshape(MEMBERS, 1, BLOCK)
    row_slots[0] = sent_slots[me]

    sums[...] = jnp.zeros_like(sums)
    tally[...] = jnp.zeros_like(tally)

    load_values.wait()
    pl.semaphore_wait(barrier, MEMBERS - 1 + 2)

    def remote(source, target, send, recv, where):
        return pltpu.make_async_remote_copy(
            src_ref=source, dst_ref=target, send_sem=send, recv_sem=recv, device_id=where, device_id_type=MESH
        )

    here = {"grp": up, "mem": me}

    def send_slots(k, _):
        to = member_at(me, k // PER_CHUNK, k % PER_CHUNK, 1)
        remote(
            sent_slots.at[to], row_slots.at[k], send_sem.at[0], slot_sem.at[0], {"grp": group, "mem": to}
        ).start()
        return 0

    def send_values(k, _):
        chunk, place = k // PER_CHUNK, k % PER_CHUNK
        to = member_at(me, chunk, place, 1)
        remote(
            vals.at[to], rows.at[chunk, place], send_sem.at[1], own_sem.at[chunk], {"grp": group, "mem": to}
        ).start()
        return 0

    lax.fori_loop(1, MEMBERS, send_slots, 0)
    lax.fori_loop(1, MEMBERS, send_values, 0)

    def landed(ref, sem):
        remote(ref, ref, send_sem.at[0], sem, here).wait_recv()

    def left(ref, sem):
        remote(ref, ref, sem, ring_sem.at[0], here).wait_send()

    def spread_slots(source):
        first = source * MEMBERS
        got = row_slots[pl.ds(first, MEMBERS)].reshape(MEMBERS, BLOCK)
        turn = lax.broadcasted_iota(jnp.int32, got.shape, 0) % 4
        flat[...] = jnp.where(lanes(got.shape) // CAP == turn, got, 0)
        quarter = MEMBERS // 4
        joined = flat[pl.ds(0, quarter, stride=4), :]
        for i in range(1, 4):
            joined = joined + flat[pl.ds(i, quarter, stride=4), :]
        lane_slots[pl.ds(pl.multiple_of(source * quarter, quarter), quarter), :] = joined
        turned = jnp.transpose(got)
        for k in range(MEMBERS):
            wide_slots[first + k] = jnp.broadcast_to(turned[:CAP, k : k + 1], (CAP, BLOCK))

    own_rows = row_slots.at[pl.ds(0, MEMBERS)]
    landed(row_slots.at[pl.ds(1, MEMBERS - 1)], slot_sem.at[0])
    remote(
        own_rows, row_slots.at[pl.ds(MEMBERS, MEMBERS)], send_sem.at[2], slot_sem.at[1], {"grp": up, "mem": me}
    ).start()
    remote(
        own_rows, row_slots.at[pl.ds(2 * MEMBERS, MEMBERS)], send_sem.at[2], slot_sem.at[2], {"grp": down, "mem": me}
    ).start()
    spread_slots(0)

    def on_own(chunk):
        @pl.when(chunk == 0)
        def _():
            load_own.wait()
            landed(rows.at[0, pl.ds(1, PER_CHUNK - 1)], own_sem.at[0])

        @pl.when(chunk > 0)
        def _():
            landed(rows.at[chunk], own_sem.at[chunk])

        remote(
            rows.at[chunk], rows.at[CHUNKS + chunk], send_sem.at[3], ring_sem.at[chunk], {"grp": up, "mem": me}
        ).start()
        remote(
            rows.at[chunk], rows.at[2 * CHUNKS + chunk], send_sem.at[3], ring_sem.at[CHUNKS + chunk],
            {"grp": down, "mem": me},
        ).start()

    some = PER_CHUNK // 2

    def on_below(chunk):
        landed(rows.at[CHUNKS + chunk], ring_sem.at[chunk])
        first = pl.ds(0, some)
        remote(
            rows.at[CHUNKS + chunk, first], rows.at[3 * CHUNKS + chunk, first], send_sem.at[4],
            ring_sem.at[2 * CHUNKS + chunk], {"grp": up, "mem": me},
        ).start()

    def on_above(chunk):
        landed(rows.at[2 * CHUNKS + chunk], ring_sem.at[CHUNKS + chunk])
        last = pl.ds(some, some)
        remote(
            rows.at[2 * CHUNKS + chunk, last], rows.at[3 * CHUNKS + chunk, last], send_sem.at[4],
            ring_sem.at[2 * CHUNKS + chunk], {"grp": down, "mem": me},
        ).start()

    def on_across(chunk):
        landed(rows.at[3 * CHUNKS + chunk], ring_sem.at[2 * CHUNKS + chunk])

    def add_piece(source, pair):
        at = source * MEMBERS + pair * PAIR
        wide = wide_slots[pl.ds(at, PAIR)].reshape(PIECE, BLOCK)
        got = rows[pl.ds(source * CHUNKS + 2 * pair, 2)].reshape(PIECE, BLOCK).astype(jnp.float32)
        second = jnp.where(wide >= HALF, got, 0.0)
        right = jnp.concatenate([got - second, second], axis=1).astype(jnp.bfloat16)
        four = lane_slots[pl.ds(source * (MEMBERS // 4) + pair * 4, 4), :]
        line = jnp.concatenate([four[i : i + 1] for i in range(4)], axis=1)
        place = lax.broadcasted_iota(jnp.int32, (HALF, PIECE), 0)
        chosen = jnp.where(place == in_half(line), 1.0, 0.0).astype(jnp.bfloat16)
        sums[...] += jnp.dot(chosen, right, preferred_element_type=jnp.float32)
        upper = lax.broadcasted_iota(jnp.int32, (MEMBERS, PIECE), 0)
        by_block = jnp.where(upper == line // BLOCK - (line < 0).astype(jnp.int32), 1.0, 0.0).astype(jnp.bfloat16)
        by_lane = jnp.where(lanes(wide.shape) == wide % BLOCK, 1.0, 0.0).astype(jnp.bfloat16)
        tally[...] += jnp.dot(by_block, by_lane, preferred_element_type=jnp.float32)

    def turn(step, _):
        source = step % GROUPS
        pair = step // GROUPS - (source + 1) // 2

        @pl.when((pair >= 0) & (pair < PIECES))
        def _():
            @pl.when((source == 1) & (pair == 0))
            def _():
                landed(row_slots.at[pl.ds(MEMBERS, MEMBERS)], slot_sem.at[1])
                landed(row_slots.at[pl.ds(2 * MEMBERS, MEMBERS)], slot_sem.at[2])
                half = MEMBERS // 2
                remote(
                    row_slots.at[pl.ds(MEMBERS, half)], row_slots.at[pl.ds(3 * MEMBERS, half)], send_sem.at[5],
                    slot_sem.at[3], {"grp": up, "mem": me},
                ).start()
                remote(
                    row_slots.at[pl.ds(2 * MEMBERS + half, half)], row_slots.at[pl.ds(3 * MEMBERS + half, half)],
                    send_sem.at[5], slot_sem.at[3], {"grp": down, "mem": me},
                ).start()

            @pl.when((source == 3) & (pair == 0))
            def _():
                landed(row_slots.at[pl.ds(3 * MEMBERS, MEMBERS)], slot_sem.at[3])

            @pl.when((source > 0) & (pair == 0))
            def _():
                spread_slots(source)

            for i in range(2):
                chunk = 2 * pair + i
                pl.when(source == 0)(functools.partial(on_own, chunk))
                pl.when(source == 1)(functools.partial(on_below, chunk))
                pl.when(source == 2)(functools.partial(on_above, chunk))
                pl.when(source == 3)(functools.partial(on_across, chunk))

            add_piece(source, pair)

        return 0

    lax.fori_loop(0, GROUPS * (PIECES + 2), turn, 0)

    scale = jnp.transpose(1.0 / jnp.maximum(tally[...], 1.0))
    for j in range(BUCKET // BLOCK):
        half, at = divmod(j * BLOCK, HALF)
        part = sums[at : at + BLOCK, half * BLOCK : (half + 1) * BLOCK]
        part = part * jnp.broadcast_to(scale[:, j : j + 1], (BLOCK, BLOCK))
        averaged[j * BLOCK : (j + 1) * BLOCK, :] = part
        mean[at : at + BLOCK, half * BLOCK : (half + 1) * BLOCK] = part.astype(jnp.bfloat16)
    store_averaged = pltpu.make_async_copy(averaged, averaged_out, out_sem.at[0])
    store_averaged.start()

    store_own = pltpu.make_async_copy(back.at[0, 0], returned_out.at[0, me], out_sem.at[1])

    def give_back(step, _):
        chunk = CHUNKS - 1 - step
        wide = wide_slots[pl.ds(chunk * PER_CHUNK, PER_CHUNK)].reshape(PER_CHUNK * CAP, BLOCK)
        offset = in_half(wide) - lanes(wide.shape)
        chosen = jnp.concatenate(
            [jnp.where(offset == i * BLOCK, 1.0, 0.0).astype(jnp.bfloat16) for i in range(HALF // BLOCK)], axis=1
        )
        both = jnp.dot(chosen, mean[...], preferred_element_type=jnp.float32)
        picked = jnp.where(wide >= HALF, both[:, BLOCK:], both[:, :BLOCK])
        picked = jnp.where(wide >= 0, picked, 0.0)
        back[chunk] = picked.astype(jnp.bfloat16).reshape(PER_CHUNK, CAP, BLOCK)

        def send_back(place, _):
            to = member_at(me, chunk, place, -1)
            remote(
                back.at[chunk, place], returned_out.at[0, me], send_sem.at[6], back_sem, {"grp": group, "mem": to}
            ).start()
            return 0

        @pl.when(chunk > 0)
        def _():
            lax.fori_loop(0, PER_CHUNK, send_back, 0)

        @pl.when(chunk == 0)
        def _():
            lax.fori_loop(1, PER_CHUNK, send_back, 0)
            store_own.start()

        return 0

    lax.fori_loop(0, CHUNKS, give_back, 0)

    left(sent_slots.at[pl.ds(0, MEMBERS - 1)], send_sem.at[0])
    left(vals.at[pl.ds(0, MEMBERS - 1)], send_sem.at[1])
    left(row_slots.at[pl.ds(0, 2 * MEMBERS)], send_sem.at[2])
    left(rows.at[pl.ds(0, 2 * CHUNKS)], send_sem.at[3])
    left(rows.at[pl.ds(0, CHUNKS)], send_sem.at[4])
    left(row_slots.at[pl.ds(0, MEMBERS)], send_sem.at[5])
    left(vals.at[pl.ds(0, MEMBERS - 1)], send_sem.at[6])
    store_own.wait()
    store_averaged.wait()
    landed(returned_out.at[0, pl.ds(0, MEMBERS - 1)], back_sem)


def per_device(values, slots, counts):
    anywhere = pl.BlockSpec(memory_space=pl.ANY)
    return pl.pallas_call(
        kernel,
        out_shape=(
            jax.ShapeDtypeStruct((BUCKET, BLOCK), jnp.float32),
            jax.ShapeDtypeStruct((1, MEMBERS, CAP, BLOCK), jnp.bfloat16),
        ),
        in_specs=[anywhere] * 3,
        out_specs=(anywhere, anywhere),
        scratch_shapes=[
            pltpu.VMEM((MEMBERS, CAP, BLOCK), jnp.bfloat16),
            pltpu.VMEM((MEMBERS, CAP), jnp.int32),
            pltpu.VMEM((1, MEMBERS), jnp.int32),
            pltpu.VMEM((MEMBERS, 1, BLOCK), jnp.int32),
            pltpu.VMEM((GROUPS * CHUNKS, PER_CHUNK, CAP, BLOCK), jnp.bfloat16),
            pltpu.VMEM((GROUPS * MEMBERS, 1, BLOCK), jnp.int32),
            pltpu.VMEM((MEMBERS, BLOCK), jnp.int32),
            pltpu.VMEM((GROUPS * MEMBERS // 4, BLOCK), jnp.int32),
            pltpu.VMEM((GROUPS * MEMBERS, CAP, BLOCK), jnp.int32),
            pltpu.VMEM((HALF, 2 * BLOCK), jnp.float32),
            pltpu.VMEM((MEMBERS, BLOCK), jnp.float32),
            pltpu.VMEM((HALF, 2 * BLOCK), jnp.bfloat16),
            pltpu.VMEM((BUCKET, BLOCK), jnp.float32),
            pltpu.VMEM((CHUNKS, PER_CHUNK, CAP, BLOCK), jnp.bfloat16),
            pltpu.SemaphoreType.DMA((4,)),
            pltpu.SemaphoreType.DMA((2,)),
            pltpu.SemaphoreType.DMA((7,)),
            pltpu.SemaphoreType.DMA((CHUNKS,)),
            pltpu.SemaphoreType.DMA((3 * CHUNKS,)),
            pltpu.SemaphoreType.DMA((4,)),
            pltpu.SemaphoreType.DMA,
        ],
        compiler_params=pltpu.CompilerParams(
            collective_id=0, has_side_effects=True, vmem_limit_bytes=60 * 2**20
        ),
        name="merge",
    )(values, slots, counts)


def solution(mesh):
    return jax.shard_map(
        per_device,
        mesh=mesh,
        in_specs=(
            P(("grp", "mem"), None, None, None),
            P(("grp", "mem"), None, None),
            P(("grp", "mem"), None),
        ),
        out_specs=(P("mem", None), P(("grp", "mem"), None, None, None)),
        check_vma=False,
    )
```

```python
import functools

import jax
import jax.numpy as jnp
from jax import lax
from jax.experimental import pallas as pl
from jax.experimental.pallas import tpu as pltpu
from jax.sharding import PartitionSpec as P

MESH = pl.DeviceIdType.MESH

GROUPS = 4
MEMBERS = 64
CAP = 32
BLOCK = 128
BUCKET = 7168
HALF = BUCKET // 2
PER_CHUNK = 8
CHUNKS = MEMBERS // PER_CHUNK
ROWS = PER_CHUNK * CAP
EARLY = 2 * PER_CHUNK

OWN, BELOW, ABOVE, ACROSS = 0, CHUNKS, 2 * CHUNKS, 3 * CHUNKS

BELOW_SLOTS, ABOVE_SLOTS, ACROSS_SLOTS = 0, 2, 4


def z_step(chunk):
    odd = lax.rem(chunk, 2)
    return odd * lax.div(chunk + 1, 2) + (1 - odd) * lax.rem(8 - lax.div(chunk, 2), 8)


def lanes(shape):
    return lax.broadcasted_iota(jnp.int32, shape, len(shape) - 1)


def in_half(slot):
    return jnp.where(slot >= HALF, slot - HALF, slot)


def kernel(
    values_in, slots_in, counts_in, averaged_out, returned_out,
    values, slots, counts, sent_slots, rows, row_slots, wide_slots, sums, tally, mean, back,
    load_sem, send_sem, own_sem, ring_sem, own_slot_sem, slot_sem, back_sem,
):
    group = lax.axis_index("grp")
    me = lax.axis_index("mem")
    above = {"grp": lax.rem(group + 1, GROUPS), "mem": me}
    below = {"grp": lax.rem(group + GROUPS - 1, GROUPS), "mem": me}
    z, x, core = lax.div(me, 8), lax.rem(lax.div(me, 2), 4), lax.rem(me, 2)
    def columns(sign):
        cores = [lax.rem(core + i, 2) for i in range(2)]
        return [2 * lax.rem(x + 4 + sign * i, 4) + cores[j] for i in range(4) for j in range(2)]

    def everyone(chunk, sign, reach):
        z_to = 8 * lax.rem(z + 8 + sign * z_step(chunk), 8)
        for place, column in enumerate(columns(sign)):
            if place:
                reach(chunk, place, z_to + column)
            else:
                pl.when(chunk > 0)(functools.partial(reach, chunk, place, z_to + column))

    def remote(source, target, send, recv, where):
        return pltpu.make_async_remote_copy(
            src_ref=source, dst_ref=target, send_sem=send, recv_sem=recv, device_id=where, device_id_type=MESH
        )

    def landed(ref, sem):
        remote(ref, ref, send_sem.at[0], sem, above).wait_recv()

    def left(ref, sem):
        remote(ref, ref, sem, back_sem, above).wait_send()

    barrier = pltpu.get_barrier_semaphore()

    def greet(chunk, place, to):
        pl.semaphore_signal(barrier, inc=1, device_id={"grp": group, "mem": to}, device_id_type=MESH)

    with jax.named_scope("greet"):
        lax.fori_loop(0, CHUNKS, lambda i, _: everyone(CHUNKS - 1 - i, 1, greet) or 0, 0)
        for other in (above, below):
            pl.semaphore_signal(barrier, inc=1, device_id=other, device_id_type=MESH)

    loads = [
        pltpu.make_async_copy(source, target, load_sem.at[i])
        for i, (source, target) in enumerate(((slots_in, slots), (counts_in, counts), (values_in, values)))
    ]
    for load in loads:
        load.start()

    with jax.named_scope("prep"):
        for load in loads[:2]:
            load.wait()
        is_valid = lax.broadcasted_iota(jnp.int32, (CAP, MEMBERS), 0) < counts[...]
        masked = jnp.where(is_valid, slots[0], -1)
        tiled = jnp.transpose(jnp.concatenate([masked] * 4, axis=0))
        sent_slots[...] = tiled.reshape(MEMBERS, 1, BLOCK)
        row_slots[0] = sent_slots[me]
        loads[2].wait()
        rows[0, 0] = values[0, me]
        sums[...] = jnp.zeros_like(sums)
        tally[...] = jnp.zeros_like(tally)

    with jax.named_scope("barrier"):
        pl.semaphore_wait(barrier, MEMBERS - 1 + 2)

    def send_slots(chunk, place, to):
        remote(
            sent_slots.at[to], row_slots.at[chunk * PER_CHUNK + place], send_sem.at[0], own_slot_sem.at[chunk],
            {"grp": group, "mem": to},
        ).start()

    def send_values(chunk, place, to):
        remote(
            values.at[0, to], rows.at[chunk, place], send_sem.at[1], own_sem.at[chunk], {"grp": group, "mem": to}
        ).start()

    with jax.named_scope("sends"):
        lax.fori_loop(0, CHUNKS, lambda i, _: everyone(i, 1, send_slots) or 0, 0)
        lax.fori_loop(0, CHUNKS, lambda i, _: everyone(i, 1, send_values) or 0, 0)

    def slot_block(source, part, side=None):
        first, count = (EARLY, MEMBERS - EARLY) if part else (0, EARLY)
        if side is not None:
            count = count // 2
            first = first + side * count
        return row_slots.at[pl.ds(source * PER_CHUNK + first, count)]

    def on_own(chunk):
        if isinstance(chunk, int) and chunk == 0:
            landed(rows.at[0, pl.ds(1, PER_CHUNK - 1)], own_sem.at[0])
        else:
            landed(rows.at[chunk], own_sem.at[chunk])
        remote(rows.at[chunk], rows.at[BELOW + chunk], send_sem.at[3], ring_sem.at[chunk], above).start()
        remote(rows.at[chunk], rows.at[ABOVE + chunk], send_sem.at[3], ring_sem.at[CHUNKS + chunk], below).start()

    some = PER_CHUNK // 2

    def on_ring(chunk):
        landed(rows.at[BELOW + chunk], ring_sem.at[chunk])
        first, last = pl.ds(0, some), pl.ds(some, some)
        remote(
            rows.at[BELOW + chunk, first], rows.at[ACROSS + chunk, first], send_sem.at[4],
            ring_sem.at[2 * CHUNKS + chunk], above,
        ).start()
        landed(rows.at[ABOVE + chunk], ring_sem.at[CHUNKS + chunk])
        remote(
            rows.at[ABOVE + chunk, last], rows.at[ACROSS + chunk, last], send_sem.at[4],
            ring_sem.at[2 * CHUNKS + chunk], below,
        ).start()

    def on_across(chunk):
        landed(rows.at[ACROSS + chunk], ring_sem.at[2 * CHUNKS + chunk])

    def widen(chunk):
        first = chunk * PER_CHUNK
        turned = jnp.transpose(row_slots[pl.ds(first, PER_CHUNK)].reshape(PER_CHUNK, BLOCK))
        for k in range(PER_CHUNK):
            wide_slots[first + k] = jnp.broadcast_to(turned[:CAP, k : k + 1], (CAP, BLOCK))

    def wide_of(chunk):
        return wide_slots[pl.ds(chunk * PER_CHUNK, PER_CHUNK)].reshape(ROWS, BLOCK)

    def lines_of(chunk):
        got = row_slots[pl.ds(chunk * PER_CHUNK, PER_CHUNK)].reshape(PER_CHUNK, BLOCK)
        quarter = lanes((1, BLOCK)) // CAP
        lines = []
        for q in range(0, PER_CHUNK, 4):
            line = got[q : q + 1]
            for i in range(1, 4):
                line = jnp.where(quarter == i, got[q + i : q + i + 1], line)
            lines.append(line)
        return lines

    def add(chunks, later):
        line = jnp.concatenate([line for chunk in chunks for line in lines_of(chunk)], axis=1)
        wide = jnp.concatenate([wide_of(chunk) for chunk in chunks], axis=0)
        got = jnp.concatenate([rows[chunk].reshape(ROWS, BLOCK) for chunk in chunks], axis=0).astype(jnp.float32)
        second = jnp.where(wide >= HALF, got, 0.0)
        right = jnp.concatenate([got - second, second], axis=1).astype(jnp.bfloat16)
        place = lax.broadcasted_iota(jnp.int32, (HALF, line.shape[1]), 0)
        chosen = jnp.where(place == in_half(line), 1.0, 0.0).astype(jnp.bfloat16)
        sums[...] += jnp.dot(chosen, right, preferred_element_type=jnp.float32)
        over = line - lax.broadcasted_iota(jnp.int32, (MEMBERS, line.shape[1]), 0) * BLOCK
        by_block = jnp.where((over >= 0) & (over < BLOCK), 1.0, 0.0).astype(jnp.bfloat16)
        by_lane = jnp.where(lanes(wide.shape) == (wide & (BLOCK - 1)), 1.0, 0.0).astype(jnp.bfloat16)
        tally[...] += jnp.dot(by_block, by_lane, preferred_element_type=jnp.float32)
        for chunk in later:
            widen(chunk)

    def own_slots(chunk):
        first = 0 if chunk else 1
        landed(row_slots.at[pl.ds(chunk * PER_CHUNK + first, PER_CHUNK - first)], own_slot_sem.at[chunk])

    def pass_slots(part):
        for source, sem, to in ((BELOW, BELOW_SLOTS, above), (ABOVE, ABOVE_SLOTS, below)):
            remote(
                slot_block(OWN, part), slot_block(source, part), send_sem.at[2], slot_sem.at[sem + part], to
            ).start()

    def ring_slots(part):
        for side, (source, sem, to) in enumerate(((BELOW, BELOW_SLOTS, above), (ABOVE, ABOVE_SLOTS, below))):
            landed(slot_block(source, part), slot_sem.at[sem + part])
            remote(
                slot_block(source, part, side), slot_block(ACROSS, part, side), send_sem.at[5],
                slot_sem.at[ACROSS_SLOTS + part], to,
            ).start()

    def across_slots(part):
        landed(slot_block(ACROSS, part), slot_sem.at[ACROSS_SLOTS + part])

    def pair(source, index):
        return [source + 2 * index, source + 2 * index + 1]

    def around(index):
        return pair(BELOW, index) + pair(ABOVE, index)

    def both(action, index):
        action(2 * index)
        action(2 * index + 1)

    def early(step, _):
        @pl.when(step == 0)
        def _():
            with jax.named_scope("w0"):
                both(own_slots, 0)
                pass_slots(0)
                both(on_own, 0)
                widen(OWN)
                widen(OWN + 1)

        @pl.when(step == 1)
        def _():
            with jax.named_scope("w1"):
                for i in range(1, CHUNKS // 2):
                    both(own_slots, i)
                pass_slots(1)
                both(on_own, 1)
                widen(OWN + 2)
                widen(OWN + 3)

        @pl.when(step == 2)
        def _():
            with jax.named_scope("w2"):
                ring_slots(0)
                widen(BELOW)
                widen(ABOVE)
                on_ring(0)

        @pl.when(step == 3)
        def _():
            with jax.named_scope("w3"):
                on_ring(1)

        ring, odd = lax.div(step, 2), lax.rem(step, 2)
        first = (1 - ring) * 2 * odd + ring * (BELOW + odd)
        second = first + 1 + ring * (ABOVE - BELOW - 1)
        next_first = ring * ((1 - odd) * (BELOW + 1) + odd * (OWN + 4))
        next_second = 1 + ring * ((1 - odd) * ABOVE + odd * (OWN + 4))
        with jax.named_scope("early"):
            add([first, second], [next_first, next_second])
        return 0

    lax.fori_loop(0, 4, early, 0)

    last = CHUNKS // 2 - 1

    def late(step, _):
        @pl.when(step <= last)
        def _():
            @pl.when(step == 2)
            def _():
                with jax.named_scope("w_own"):
                    both(on_own, 2)
                    ring_slots(1)

            with jax.named_scope("own"):
                add(pair(OWN, step), around(step - 1) + pair(OWN, last))

        @pl.when(step <= last + 1)
        def _():
            with jax.named_scope("w_ring"):
                both(on_ring, step - 1)

                for part in range(2):
                    pl.when(step == 2 + part)(functools.partial(across_slots, part))

            with jax.named_scope("ring"):
                add(around(step - 1), pair(ACROSS, step - 2))

        @pl.when(step == 2)
        def _():
            with jax.named_scope("w_own3"):
                both(on_own, last)

        with jax.named_scope("w_across"):
            both(on_across, step - 2)
        with jax.named_scope("across"):
            after = jnp.where(step > 2, jnp.minimum(step - 1, last), 0)
            add(pair(ACROSS, step - 2), around(jnp.minimum(step, last)) + pair(ACROSS, after))
        return 0

    lax.fori_loop(2, last + 3, late, 0)

    with jax.named_scope("mean"):
        scale = jnp.transpose(1.0 / jnp.maximum(tally[...], 1.0))
        for j in range(BUCKET // BLOCK):
            side, at = divmod(j * BLOCK, HALF)
            part = sums[at : at + BLOCK, side * BLOCK : (side + 1) * BLOCK]
            part = part * jnp.broadcast_to(scale[:, j : j + 1], (BLOCK, BLOCK))
            averaged_out[j * BLOCK : (j + 1) * BLOCK, :] = part
            mean[at : at + BLOCK, side * BLOCK : (side + 1) * BLOCK] = part.astype(jnp.bfloat16)

    def give_back(step, _):
        chunk = CHUNKS - 1 - step
        with jax.named_scope("gather"):
            wide = wide_of(chunk)
            offset = in_half(wide) - lanes(wide.shape)
            chosen = jnp.concatenate(
                [jnp.where(offset == i * BLOCK, 1.0, 0.0).astype(jnp.bfloat16) for i in range(HALF // BLOCK)], axis=1
            )
            sides = jnp.dot(chosen, mean[...], preferred_element_type=jnp.float32)
            picked = jnp.where(wide >= HALF, sides[:, BLOCK:], sides[:, :BLOCK])
            picked = jnp.where(wide >= 0, picked, 0.0)
            back[chunk] = picked.astype(jnp.bfloat16).reshape(PER_CHUNK, CAP, BLOCK)

        def send_back(chunk, place, to):
            remote(
                back.at[chunk, place], returned_out.at[0, me], send_sem.at[6], back_sem, {"grp": group, "mem": to}
            ).start()

        with jax.named_scope("sendback"):
            everyone(chunk, -1, send_back)

        return 0

    lax.fori_loop(0, CHUNKS, give_back, 0)
    returned_out[0, me] = back[0, 0]

    most = pl.ds(0, MEMBERS - 1)
    with jax.named_scope("lefts"):
        left(sent_slots.at[most], send_sem.at[0])
        left(values.at[0, most], send_sem.at[1])
        left(row_slots.at[pl.ds(0, 2 * MEMBERS)], send_sem.at[2])
        left(rows.at[pl.ds(0, 2 * CHUNKS)], send_sem.at[3])
        left(rows.at[pl.ds(0, CHUNKS)], send_sem.at[4])
        left(row_slots.at[pl.ds(0, MEMBERS)], send_sem.at[5])
        left(values.at[0, most], send_sem.at[6])
    with jax.named_scope("waitback"):
        landed(returned_out.at[0, most], back_sem)


PARTS = 8


def hand_over(averaged, returned, averaged_out, returned_out, sem):
    part = BUCKET // PARTS
    copies = [pltpu.make_async_copy(returned, returned_out, sem.at[PARTS])]
    for i in range(PARTS):
        at = pl.ds(i * part, part)
        copies.append(pltpu.make_async_copy(averaged.at[at], averaged_out.at[at], sem.at[i]))
    for copy in copies:
        copy.start()
    for copy in copies:
        copy.wait()


def per_device(values, slots, counts):
    in_hbm = pl.BlockSpec(memory_space=pltpu.HBM)
    in_vmem = pl.BlockSpec(memory_space=pltpu.VMEM)
    operands = [pltpu.with_memory_space_constraint(x, pltpu.HBM) for x in (values, jnp.swapaxes(slots, 1, 2), counts)]
    results = pl.pallas_call(
        kernel,
        out_shape=(
            jax.ShapeDtypeStruct((BUCKET, BLOCK), jnp.float32),
            jax.ShapeDtypeStruct((1, MEMBERS, CAP, BLOCK), jnp.bfloat16),
        ),
        in_specs=[in_hbm] * 3,
        out_specs=(in_vmem, in_vmem),
        scratch_shapes=[
            pltpu.VMEM((1, MEMBERS, CAP, BLOCK), jnp.bfloat16),
            pltpu.VMEM((1, CAP, MEMBERS), jnp.int32),
            pltpu.VMEM((1, MEMBERS), jnp.int32),
            pltpu.VMEM((MEMBERS, 1, BLOCK), jnp.int32),
            pltpu.VMEM((GROUPS * CHUNKS, PER_CHUNK, CAP, BLOCK), jnp.bfloat16),
            pltpu.VMEM((GROUPS * MEMBERS, 1, BLOCK), jnp.int32),
            pltpu.VMEM((GROUPS * MEMBERS, CAP, BLOCK), jnp.int32),
            pltpu.VMEM((HALF, 2 * BLOCK), jnp.float32),
            pltpu.VMEM((MEMBERS, BLOCK), jnp.float32),
            pltpu.VMEM((HALF, 2 * BLOCK), jnp.bfloat16),
            pltpu.VMEM((CHUNKS, PER_CHUNK, CAP, BLOCK), jnp.bfloat16),
            pltpu.SemaphoreType.DMA((3,)),
            pltpu.SemaphoreType.DMA((7,)),
            pltpu.SemaphoreType.DMA((CHUNKS,)),
            pltpu.SemaphoreType.DMA((3 * CHUNKS,)),
            pltpu.SemaphoreType.DMA((CHUNKS,)),
            pltpu.SemaphoreType.DMA((6,)),
            pltpu.SemaphoreType.DMA,
        ],
        compiler_params=pltpu.CompilerParams(
            collective_id=0, has_side_effects=True, vmem_limit_bytes=40 * 2**20
        ),
        name="merge",
    )(*operands)
    return pl.pallas_call(
        hand_over,
        out_shape=[jax.ShapeDtypeStruct(x.shape, x.dtype) for x in results],
        in_specs=[in_vmem, in_vmem],
        out_specs=[in_hbm, in_hbm],
        scratch_shapes=[pltpu.SemaphoreType.DMA((PARTS + 1,))],
        compiler_params=pltpu.CompilerParams(vmem_limit_bytes=2**20),
        name="hand_over",
    )(*results)


def solution(mesh):
    return jax.shard_map(
        per_device,
        mesh=mesh,
        in_specs=(
            P(("grp", "mem"), None, None, None),
            P(("grp", "mem"), None, None),
            P(("grp", "mem"), None),
        ),
        out_specs=(P("mem", None), P(("grp", "mem"), None, None, None)),
        check_vma=False,
    )
```

```python
import functools

import jax
import jax.numpy as jnp
from jax import lax
from jax.experimental import pallas as pl
from jax.experimental.pallas import tpu as pltpu
from jax.sharding import PartitionSpec as P

MESH = pl.DeviceIdType.MESH

GROUPS = 4
MEMBERS = 64
CAP = 32
BLOCK = 128
BUCKET = 7168
HALF = BUCKET // 2
PER_CHUNK = 8
CHUNKS = MEMBERS // PER_CHUNK
ROWS = PER_CHUNK * CAP
EARLY = 2 * PER_CHUNK

OWN, BELOW, ABOVE, ACROSS = 0, CHUNKS, 2 * CHUNKS, 3 * CHUNKS

BELOW_SLOTS, ABOVE_SLOTS, ACROSS_SLOTS = 0, 2, 4


def z_step(chunk):
    odd = lax.rem(chunk, 2)
    return odd * lax.div(chunk + 1, 2) + (1 - odd) * lax.rem(8 - lax.div(chunk, 2), 8)


def lanes(shape):
    return lax.broadcasted_iota(jnp.int32, shape, len(shape) - 1)


def in_half(slot):
    return jnp.where(slot >= HALF, slot - HALF, slot)


def kernel(
    values_in, slots_in, counts_in, averaged_out, returned_out,
    values, slots, counts, sent_slots, rows, row_slots, wide_slots, sums, tally, mean, back,
    load_sem, send_sem, own_sem, ring_sem, own_slot_sem, slot_sem, back_sem,
):
    group = lax.axis_index("grp")
    me = lax.axis_index("mem")
    above = {"grp": lax.rem(group + 1, GROUPS), "mem": me}
    below = {"grp": lax.rem(group + GROUPS - 1, GROUPS), "mem": me}
    z, x, core = lax.div(me, 8), lax.rem(lax.div(me, 2), 4), lax.rem(me, 2)
    def columns(sign):
        cores = [lax.rem(core + i, 2) for i in range(2)]
        return [2 * lax.rem(x + 4 + sign * i, 4) + cores[j] for i in range(4) for j in range(2)]

    def everyone(chunk, sign, reach):
        z_to = 8 * lax.rem(z + 8 + sign * z_step(chunk), 8)
        for place, column in enumerate(columns(sign)):
            if place:
                reach(chunk, place, z_to + column)
            else:
                pl.when(chunk > 0)(functools.partial(reach, chunk, place, z_to + column))

    def remote(source, target, send, recv, where):
        return pltpu.make_async_remote_copy(
            src_ref=source, dst_ref=target, send_sem=send, recv_sem=recv, device_id=where, device_id_type=MESH
        )

    def landed(ref, sem):
        remote(ref, ref, send_sem.at[0], sem, above).wait_recv()

    def left(ref, sem):
        remote(ref, ref, sem, back_sem, above).wait_send()

    barrier = pltpu.get_barrier_semaphore()

    def greet(chunk, place, to):
        pl.semaphore_signal(barrier, inc=1, device_id={"grp": group, "mem": to}, device_id_type=MESH)

    with jax.named_scope("greet"):
        lax.fori_loop(0, CHUNKS, lambda i, _: everyone(CHUNKS - 1 - i, 1, greet) or 0, 0)
        for other in (above, below):
            pl.semaphore_signal(barrier, inc=1, device_id=other, device_id_type=MESH)

    loads = [
        pltpu.make_async_copy(source, target, load_sem.at[i])
        for i, (source, target) in enumerate(((slots_in, slots), (counts_in, counts), (values_in, values)))
    ]
    for load in loads:
        load.start()

    with jax.named_scope("prep"):
        for load in loads[:2]:
            load.wait()
        is_valid = lax.broadcasted_iota(jnp.int32, (CAP, MEMBERS), 0) < counts[...]
        masked = jnp.where(is_valid, slots[0], -1)
        tiled = jnp.transpose(jnp.concatenate([masked] * 4, axis=0))
        sent_slots[...] = tiled.reshape(MEMBERS, 1, BLOCK)
        row_slots[0] = sent_slots[me]
        loads[2].wait()
        rows[0, 0] = values[0, me]
        sums[...] = jnp.zeros_like(sums)
        tally[...] = jnp.zeros_like(tally)

    with jax.named_scope("barrier"):
        pl.semaphore_wait(barrier, MEMBERS - 1 + 2)

    def send_slots(chunk, place, to):
        remote(
            sent_slots.at[to], row_slots.at[chunk * PER_CHUNK + place], send_sem.at[0], own_slot_sem.at[chunk],
            {"grp": group, "mem": to},
        ).start()

    def send_values(chunk, place, to):
        remote(
            values.at[0, to], rows.at[chunk, place], send_sem.at[1], own_sem.at[chunk], {"grp": group, "mem": to}
        ).start()

    with jax.named_scope("sends"):
        lax.fori_loop(0, CHUNKS, lambda i, _: everyone(i, 1, send_slots) or 0, 0)
        lax.fori_loop(0, CHUNKS, lambda i, _: everyone(i, 1, send_values) or 0, 0)

    def slot_block(source, part, side=None):
        first, count = (EARLY, MEMBERS - EARLY) if part else (0, EARLY)
        if side is not None:
            count = count // 2
            first = first + side * count
        return row_slots.at[pl.ds(source * PER_CHUNK + first, count)]

    def on_own(chunk):
        if isinstance(chunk, int) and chunk == 0:
            landed(rows.at[0, pl.ds(1, PER_CHUNK - 1)], own_sem.at[0])
        else:
            landed(rows.at[chunk], own_sem.at[chunk])
        remote(rows.at[chunk], rows.at[BELOW + chunk], send_sem.at[3], ring_sem.at[chunk], above).start()
        remote(rows.at[chunk], rows.at[ABOVE + chunk], send_sem.at[3], ring_sem.at[CHUNKS + chunk], below).start()

    some = PER_CHUNK // 2

    def on_ring(chunk):
        landed(rows.at[BELOW + chunk], ring_sem.at[chunk])
        first, last = pl.ds(0, some), pl.ds(some, some)
        remote(
            rows.at[BELOW + chunk, first], rows.at[ACROSS + chunk, first], send_sem.at[4],
            ring_sem.at[2 * CHUNKS + chunk], above,
        ).start()
        landed(rows.at[ABOVE + chunk], ring_sem.at[CHUNKS + chunk])
        remote(
            rows.at[ABOVE + chunk, last], rows.at[ACROSS + chunk, last], send_sem.at[4],
            ring_sem.at[2 * CHUNKS + chunk], below,
        ).start()

    def on_across(chunk):
        landed(rows.at[ACROSS + chunk], ring_sem.at[2 * CHUNKS + chunk])

    def widen(chunk):
        first = chunk * PER_CHUNK
        turned = jnp.transpose(row_slots[pl.ds(first, PER_CHUNK)].reshape(PER_CHUNK, BLOCK))
        for k in range(PER_CHUNK):
            wide_slots[first + k] = jnp.broadcast_to(turned[:CAP, k : k + 1], (CAP, BLOCK))

    def wide_of(chunk):
        return wide_slots[pl.ds(chunk * PER_CHUNK, PER_CHUNK)].reshape(ROWS, BLOCK)

    def lines_of(chunk):
        got = row_slots[pl.ds(chunk * PER_CHUNK, PER_CHUNK)].reshape(PER_CHUNK, BLOCK)
        quarter = lanes((1, BLOCK)) // CAP
        lines = []
        for q in range(0, PER_CHUNK, 4):
            line = got[q : q + 1]
            for i in range(1, 4):
                line = jnp.where(quarter == i, got[q + i : q + i + 1], line)
            lines.append(line)
        return lines

    def add(chunks, later):
        line = jnp.concatenate([line for chunk in chunks for line in lines_of(chunk)], axis=1)
        wide = jnp.concatenate([wide_of(chunk) for chunk in chunks], axis=0)
        over = line - lax.broadcasted_iota(jnp.int32, (MEMBERS, line.shape[1]), 0) * BLOCK
        by_block = jnp.where((over >= 0) & (over < BLOCK), 1.0, 0.0).astype(jnp.bfloat16)
        by_lane = jnp.where(lanes(wide.shape) == (wide & (BLOCK - 1)), 1.0, 0.0).astype(jnp.bfloat16)
        tally[...] += jnp.dot(by_block, by_lane, preferred_element_type=jnp.float32)
        got = jnp.concatenate([rows[chunk].reshape(ROWS, BLOCK) for chunk in chunks], axis=0).astype(jnp.float32)
        second = jnp.where(wide >= HALF, got, 0.0)
        right = jnp.concatenate([got - second, second], axis=1).astype(jnp.bfloat16)
        place = lax.broadcasted_iota(jnp.int32, (HALF, line.shape[1]), 0)
        chosen = jnp.where(place == in_half(line), 1.0, 0.0).astype(jnp.bfloat16)
        sums[...] += jnp.dot(chosen, right, preferred_element_type=jnp.float32)
        for chunk in later:
            widen(chunk)

    def finish():
        scale = jnp.transpose(1.0 / jnp.maximum(tally[...], 1.0))
        for j in range(HALF // BLOCK):
            at = j * BLOCK
            for side in range(2):
                column = side * (HALF // BLOCK) + j
                part = sums[at : at + BLOCK, side * BLOCK : (side + 1) * BLOCK]
                part = part * jnp.broadcast_to(scale[:, column : column + 1], (BLOCK, BLOCK))
                averaged_out[side * HALF + at : side * HALF + at + BLOCK, :] = part
                mean[at : at + BLOCK, side * BLOCK : (side + 1) * BLOCK] = part.astype(jnp.bfloat16)

    def own_slots(chunk):
        first = 0 if chunk else 1
        landed(row_slots.at[pl.ds(chunk * PER_CHUNK + first, PER_CHUNK - first)], own_slot_sem.at[chunk])

    def pass_slots(part):
        for source, sem, to in ((BELOW, BELOW_SLOTS, above), (ABOVE, ABOVE_SLOTS, below)):
            remote(
                slot_block(OWN, part), slot_block(source, part), send_sem.at[2], slot_sem.at[sem + part], to
            ).start()

    def ring_slots(part):
        for side, (source, sem, to) in enumerate(((BELOW, BELOW_SLOTS, above), (ABOVE, ABOVE_SLOTS, below))):
            landed(slot_block(source, part), slot_sem.at[sem + part])
            remote(
                slot_block(source, part, side), slot_block(ACROSS, part, side), send_sem.at[5],
                slot_sem.at[ACROSS_SLOTS + part], to,
            ).start()

    def across_slots(part):
        landed(slot_block(ACROSS, part), slot_sem.at[ACROSS_SLOTS + part])

    def pair(source, index):
        return [source + 2 * index, source + 2 * index + 1]

    def around(index):
        return pair(BELOW, index) + pair(ABOVE, index)

    def both(action, index):
        action(2 * index)
        action(2 * index + 1)

    def pick(step, *values):
        at = values[0]
        for k in range(1, len(values)):
            at = jnp.where(step == k, values[k], at)
        return at

    def early(step, _):
        @pl.when(step == 0)
        def _():
            with jax.named_scope("w0"):
                both(own_slots, 0)
                pass_slots(0)
                both(on_own, 0)
                widen(OWN)
                widen(OWN + 1)

        @pl.when(step == 1)
        def _():
            with jax.named_scope("w1"):
                for i in range(1, CHUNKS // 2):
                    both(own_slots, i)
                pass_slots(1)
                both(on_own, 1)
                widen(OWN + 2)
                widen(OWN + 3)

        @pl.when(step == 2)
        def _():
            with jax.named_scope("w2"):
                ring_slots(0)
                widen(BELOW)
                widen(ABOVE)
                on_ring(0)

        @pl.when(step == 3)
        def _():
            with jax.named_scope("w3"):
                on_ring(1)
                ring_slots(1)

        chunks = zip(pair(OWN, 0), pair(OWN, 1), (BELOW, ABOVE), (BELOW + 1, ABOVE + 1))
        later = zip(pair(OWN, 0) * 2, pair(OWN, 0) * 2, (BELOW + 1, ABOVE + 1) * 2, around(1))
        with jax.named_scope("early"):
            add([pick(step, *options) for options in chunks], [pick(step, *options) for options in later])
        return 0

    lax.fori_loop(0, 4, early, 0)

    last = CHUNKS // 2 - 1
    none = [0] * 4

    def late(step, _):
        @pl.when((step == 0) | (step == 3) | (step == 4))
        def _():
            @pl.when(step == 0)
            def _():
                with jax.named_scope("wr0"):
                    on_own(4)
                    both(on_ring, 1)

            @pl.when(step > 0)
            def _():
                with jax.named_scope("wr"):
                    both(on_ring, step - 1)
                    pl.when(step == 3)(functools.partial(across_slots, 1))

            chunks = zip(around(1), none, none, around(2), around(3))
            later = zip(pair(OWN, 2) * 2, none, none, around(3), pair(ACROSS, 1) * 2)
            with jax.named_scope("ring"):
                add([pick(step, *options) for options in chunks], [pick(step, *options) for options in later])

        @pl.when(step != 3)
        def _():
            @pl.when(step < 3)
            def _():
                with jax.named_scope("wo"):
                    on_own(5 + step)
                    pl.when(step == 0)(functools.partial(across_slots, 0))
                    pl.when(step == 1)(functools.partial(both, on_across, 0))

            @pl.when(step > 3)
            def _():
                with jax.named_scope("wa"):
                    both(on_across, step - 3)

            chunks = zip(pair(OWN, 2), pair(ACROSS, 0), pair(OWN, 3), (0, 0), pair(ACROSS, 1), pair(ACROSS, 2))
            later = zip(pair(ACROSS, 0) * 2, pair(OWN, 3) * 2, around(2), none, pair(ACROSS, 2) * 2, pair(ACROSS, 3) * 2)
            with jax.named_scope("single"):
                add([pick(step, *options) for options in chunks], [pick(step, *options) for options in later])

        return 0

    lax.fori_loop(0, 6, late, 0)
    with jax.named_scope("w_last"):
        both(on_across, last)
    with jax.named_scope("last"):
        add(pair(ACROSS, last), [])
        finish()

    def give_back(step, _):
        chunk = CHUNKS - 1 - step
        with jax.named_scope("gather"):
            wide = wide_of(chunk)
            offset = in_half(wide) - lanes(wide.shape)
            chosen = jnp.concatenate(
                [jnp.where(offset == i * BLOCK, 1.0, 0.0).astype(jnp.bfloat16) for i in range(HALF // BLOCK)], axis=1
            )
            sides = jnp.dot(chosen, mean[...], preferred_element_type=jnp.float32)
            picked = jnp.where(wide >= HALF, sides[:, BLOCK:], sides[:, :BLOCK])
            picked = jnp.where(wide >= 0, picked, 0.0)
            back[chunk] = picked.astype(jnp.bfloat16).reshape(PER_CHUNK, CAP, BLOCK)

        def send_back(chunk, place, to):
            remote(
                back.at[chunk, place], returned_out.at[0, me], send_sem.at[6], back_sem, {"grp": group, "mem": to}
            ).start()

        with jax.named_scope("sendback"):
            everyone(chunk, -1, send_back)

        return 0

    lax.fori_loop(0, CHUNKS, give_back, 0)
    returned_out[0, me] = back[0, 0]

    most = pl.ds(0, MEMBERS - 1)
    with jax.named_scope("lefts"):
        left(sent_slots.at[most], send_sem.at[0])
        left(values.at[0, most], send_sem.at[1])
        left(row_slots.at[pl.ds(0, 2 * MEMBERS)], send_sem.at[2])
        left(rows.at[pl.ds(0, 2 * CHUNKS)], send_sem.at[3])
        left(rows.at[pl.ds(0, CHUNKS)], send_sem.at[4])
        left(row_slots.at[pl.ds(0, MEMBERS)], send_sem.at[5])
        left(values.at[0, most], send_sem.at[6])
    with jax.named_scope("waitback"):
        landed(returned_out.at[0, most], back_sem)


PARTS = 8


def hand_over(averaged, returned, averaged_out, returned_out, sem):
    part = BUCKET // PARTS
    copies = [pltpu.make_async_copy(returned, returned_out, sem.at[PARTS])]
    for i in range(PARTS):
        at = pl.ds(i * part, part)
        copies.append(pltpu.make_async_copy(averaged.at[at], averaged_out.at[at], sem.at[i]))
    for copy in copies:
        copy.start()
    for copy in copies:
        copy.wait()


def per_device(values, slots, counts):
    in_hbm = pl.BlockSpec(memory_space=pltpu.HBM)
    in_vmem = pl.BlockSpec(memory_space=pltpu.VMEM)
    operands = [pltpu.with_memory_space_constraint(x, pltpu.HBM) for x in (values, jnp.swapaxes(slots, 1, 2), counts)]
    results = pl.pallas_call(
        kernel,
        out_shape=(
            jax.ShapeDtypeStruct((BUCKET, BLOCK), jnp.float32),
            jax.ShapeDtypeStruct((1, MEMBERS, CAP, BLOCK), jnp.bfloat16),
        ),
        in_specs=[in_hbm] * 3,
        out_specs=(in_vmem, in_vmem),
        scratch_shapes=[
            pltpu.VMEM((1, MEMBERS, CAP, BLOCK), jnp.bfloat16),
            pltpu.VMEM((1, CAP, MEMBERS), jnp.int32),
            pltpu.VMEM((1, MEMBERS), jnp.int32),
            pltpu.VMEM((MEMBERS, 1, BLOCK), jnp.int32),
            pltpu.VMEM((GROUPS * CHUNKS, PER_CHUNK, CAP, BLOCK), jnp.bfloat16),
            pltpu.VMEM((GROUPS * MEMBERS, 1, BLOCK), jnp.int32),
            pltpu.VMEM((GROUPS * MEMBERS, CAP, BLOCK), jnp.int32),
            pltpu.VMEM((HALF, 2 * BLOCK), jnp.float32),
            pltpu.VMEM((MEMBERS, BLOCK), jnp.float32),
            pltpu.VMEM((HALF, 2 * BLOCK), jnp.bfloat16),
            pltpu.VMEM((CHUNKS, PER_CHUNK, CAP, BLOCK), jnp.bfloat16),
            pltpu.SemaphoreType.DMA((3,)),
            pltpu.SemaphoreType.DMA((7,)),
            pltpu.SemaphoreType.DMA((CHUNKS,)),
            pltpu.SemaphoreType.DMA((3 * CHUNKS,)),
            pltpu.SemaphoreType.DMA((CHUNKS,)),
            pltpu.SemaphoreType.DMA((6,)),
            pltpu.SemaphoreType.DMA,
        ],
        compiler_params=pltpu.CompilerParams(
            collective_id=0, has_side_effects=True, vmem_limit_bytes=40 * 2**20
        ),
        name="merge",
    )(*operands)
    return pl.pallas_call(
        hand_over,
        out_shape=[jax.ShapeDtypeStruct(x.shape, x.dtype) for x in results],
        in_specs=[in_vmem, in_vmem],
        out_specs=[in_hbm, in_hbm],
        scratch_shapes=[pltpu.SemaphoreType.DMA((PARTS + 1,))],
        compiler_params=pltpu.CompilerParams(vmem_limit_bytes=2**20),
        name="hand_over",
    )(*results)


def solution(mesh):
    return jax.shard_map(
        per_device,
        mesh=mesh,
        in_specs=(
            P(("grp", "mem"), None, None, None),
            P(("grp", "mem"), None, None),
            P(("grp", "mem"), None),
        ),
        out_specs=(P("mem", None), P(("grp", "mem"), None, None, None)),
        check_vma=False,
    )
```

```python
import functools

import jax
import jax.numpy as jnp
from jax import lax
from jax.experimental import pallas as pl
from jax.experimental.pallas import tpu as pltpu
from jax.sharding import PartitionSpec as P

MESH = pl.DeviceIdType.MESH

GROUPS = 4
MEMBERS = 64
CAP = 32
BLOCK = 128
BUCKET = 7168
HALF = BUCKET // 2
PER_CHUNK = 8
CHUNKS = MEMBERS // PER_CHUNK
ROWS = PER_CHUNK * CAP
EARLY = 2 * PER_CHUNK

OWN, BELOW, ABOVE, ACROSS = 0, CHUNKS, 2 * CHUNKS, 3 * CHUNKS

BELOW_SLOTS, ABOVE_SLOTS, ACROSS_SLOTS = 0, 2, 4


def z_step(chunk):
    odd = lax.rem(chunk, 2)
    return odd * lax.div(chunk + 1, 2) + (1 - odd) * lax.rem(8 - lax.div(chunk, 2), 8)


def lanes(shape):
    return lax.broadcasted_iota(jnp.int32, shape, len(shape) - 1)


def in_half(slot):
    return jnp.where(slot >= HALF, slot - HALF, slot)


def kernel(
    values_in, slots_in, counts_in, averaged_out, returned_out,
    values, slots, counts, sent_slots, rows, row_slots, wide_slots, sums, tally, mean, back,
    load_sem, send_sem, own_sem, ring_sem, own_slot_sem, slot_sem, back_sem,
):
    group = lax.axis_index("grp")
    me = lax.axis_index("mem")
    above = {"grp": lax.rem(group + 1, GROUPS), "mem": me}
    below = {"grp": lax.rem(group + GROUPS - 1, GROUPS), "mem": me}
    across = {"grp": lax.rem(group + 2, GROUPS), "mem": me}
    z, x, core = lax.div(me, 8), lax.rem(lax.div(me, 2), 4), lax.rem(me, 2)
    def columns(sign):
        cores = [lax.rem(core + i, 2) for i in range(2)]
        return [2 * lax.rem(x + 4 + sign * i, 4) + cores[j] for i in range(4) for j in range(2)]

    def everyone(chunk, sign, reach):
        z_to = 8 * lax.rem(z + 8 + sign * z_step(chunk), 8)
        for place, column in enumerate(columns(sign)):
            if place:
                reach(chunk, place, z_to + column)
            else:
                pl.when(chunk > 0)(functools.partial(reach, chunk, place, z_to + column))

    def remote(source, target, send, recv, where):
        return pltpu.make_async_remote_copy(
            src_ref=source, dst_ref=target, send_sem=send, recv_sem=recv, device_id=where, device_id_type=MESH
        )

    def landed(ref, sem):
        remote(ref, ref, send_sem.at[0], sem, above).wait_recv()

    def left(ref, sem):
        remote(ref, ref, sem, back_sem, above).wait_send()

    barrier = pltpu.get_barrier_semaphore()

    def greet(chunk, place, to):
        pl.semaphore_signal(barrier, inc=1, device_id={"grp": group, "mem": to}, device_id_type=MESH)

    with jax.named_scope("greet"):
        lax.fori_loop(0, CHUNKS, lambda i, _: everyone(CHUNKS - 1 - i, 1, greet) or 0, 0)
        for other in (above, below, across):
            pl.semaphore_signal(barrier, inc=1, device_id=other, device_id_type=MESH)

    loads = [
        pltpu.make_async_copy(source, target, load_sem.at[i])
        for i, (source, target) in enumerate(((slots_in, slots), (counts_in, counts), (values_in, values)))
    ]
    for load in loads:
        load.start()

    with jax.named_scope("prep"):
        for load in loads[:2]:
            load.wait()
        is_valid = lax.broadcasted_iota(jnp.int32, (CAP, MEMBERS), 0) < counts[...]
        masked = jnp.where(is_valid, slots[0], -1)
        tiled = jnp.transpose(jnp.concatenate([masked] * 4, axis=0))
        sent_slots[...] = tiled.reshape(MEMBERS, 1, BLOCK)
        row_slots[0] = sent_slots[me]
        loads[2].wait()
        rows[0, 0] = values[0, me]
        sums[...] = jnp.zeros_like(sums)
        tally[...] = jnp.zeros_like(tally)

    with jax.named_scope("barrier"):
        pl.semaphore_wait(barrier, MEMBERS - 1 + GROUPS - 1)

    def send_slots(chunk, place, to):
        remote(
            sent_slots.at[to], row_slots.at[chunk * PER_CHUNK + place], send_sem.at[0], own_slot_sem.at[chunk],
            {"grp": group, "mem": to},
        ).start()

    def send_values(chunk, place, to):
        remote(
            values.at[0, to], rows.at[chunk, place], send_sem.at[1], own_sem.at[chunk], {"grp": group, "mem": to}
        ).start()

    with jax.named_scope("sends"):
        lax.fori_loop(0, CHUNKS, lambda i, _: everyone(i, 1, send_slots) or 0, 0)
        lax.fori_loop(0, CHUNKS, lambda i, _: everyone(i, 1, send_values) or 0, 0)

    def slot_block(source, part, side=None):
        first, count = (EARLY, MEMBERS - EARLY) if part else (0, EARLY)
        if side is not None:
            count = count // 2
            first = first + side * count
        return row_slots.at[pl.ds(source * PER_CHUNK + first, count)]

    def on_own(chunk):
        if isinstance(chunk, int) and chunk == 0:
            landed(rows.at[0, pl.ds(1, PER_CHUNK - 1)], own_sem.at[0])
        else:
            landed(rows.at[chunk], own_sem.at[chunk])
        remote(rows.at[chunk], rows.at[BELOW + chunk], send_sem.at[3], ring_sem.at[chunk], above).start()
        remote(rows.at[chunk], rows.at[ABOVE + chunk], send_sem.at[3], ring_sem.at[CHUNKS + chunk], below).start()
        if isinstance(chunk, int) and chunk == CHUNKS - 1:
            remote(
                rows.at[chunk], rows.at[ACROSS + chunk], send_sem.at[3], ring_sem.at[2 * CHUNKS + chunk], across
            ).start()

    some = PER_CHUNK // 2

    def on_ring(chunk):
        if isinstance(chunk, int) and chunk == CHUNKS - 1:
            landed(rows.at[BELOW + chunk], ring_sem.at[chunk])
            landed(rows.at[ABOVE + chunk], ring_sem.at[CHUNKS + chunk])
            return
        landed(rows.at[BELOW + chunk], ring_sem.at[chunk])
        first, last = pl.ds(0, some), pl.ds(some, some)
        remote(
            rows.at[BELOW + chunk, first], rows.at[ACROSS + chunk, first], send_sem.at[4],
            ring_sem.at[2 * CHUNKS + chunk], above,
        ).start()
        landed(rows.at[ABOVE + chunk], ring_sem.at[CHUNKS + chunk])
        remote(
            rows.at[ABOVE + chunk, last], rows.at[ACROSS + chunk, last], send_sem.at[4],
            ring_sem.at[2 * CHUNKS + chunk], below,
        ).start()

    def on_across(chunk):
        landed(rows.at[ACROSS + chunk], ring_sem.at[2 * CHUNKS + chunk])

    def widen(chunk):
        first = chunk * PER_CHUNK
        turned = jnp.transpose(row_slots[pl.ds(first, PER_CHUNK)].reshape(PER_CHUNK, BLOCK))
        for k in range(PER_CHUNK):
            wide_slots[first + k] = jnp.broadcast_to(turned[:CAP, k : k + 1], (CAP, BLOCK))

    def wide_of(chunk):
        return wide_slots[pl.ds(chunk * PER_CHUNK, PER_CHUNK)].reshape(ROWS, BLOCK)

    def lines_of(chunk):
        got = row_slots[pl.ds(chunk * PER_CHUNK, PER_CHUNK)].reshape(PER_CHUNK, BLOCK)
        quarter = lanes((1, BLOCK)) // CAP
        lines = []
        for q in range(0, PER_CHUNK, 4):
            line = got[q : q + 1]
            for i in range(1, 4):
                line = jnp.where(quarter == i, got[q + i : q + i + 1], line)
            lines.append(line)
        return lines

    def add(chunks, later):
        line = jnp.concatenate([line for chunk in chunks for line in lines_of(chunk)], axis=1)
        wide = jnp.concatenate([wide_of(chunk) for chunk in chunks], axis=0)
        over = line - lax.broadcasted_iota(jnp.int32, (MEMBERS, line.shape[1]), 0) * BLOCK
        by_block = jnp.where((over >= 0) & (over < BLOCK), 1.0, 0.0).astype(jnp.bfloat16)
        by_lane = jnp.where(lanes(wide.shape) == (wide & (BLOCK - 1)), 1.0, 0.0).astype(jnp.bfloat16)
        tally[...] += jnp.dot(by_block, by_lane, preferred_element_type=jnp.float32)
        got = jnp.concatenate([rows[chunk].reshape(ROWS, BLOCK) for chunk in chunks], axis=0).astype(jnp.float32)
        second = jnp.where(wide >= HALF, got, 0.0)
        right = jnp.concatenate([got - second, second], axis=1).astype(jnp.bfloat16)
        place = lax.broadcasted_iota(jnp.int32, (HALF, line.shape[1]), 0)
        chosen = jnp.where(place == in_half(line), 1.0, 0.0).astype(jnp.bfloat16)
        sums[...] += jnp.dot(chosen, right, preferred_element_type=jnp.float32)
        for chunk in later:
            widen(chunk)

    def finish():
        scale = jnp.transpose(1.0 / jnp.maximum(tally[...], 1.0))
        for j in range(HALF // BLOCK):
            at = j * BLOCK
            for side in range(2):
                column = side * (HALF // BLOCK) + j
                part = sums[at : at + BLOCK, side * BLOCK : (side + 1) * BLOCK]
                part = part * jnp.broadcast_to(scale[:, column : column + 1], (BLOCK, BLOCK))
                averaged_out[side * HALF + at : side * HALF + at + BLOCK, :] = part
                mean[at : at + BLOCK, side * BLOCK : (side + 1) * BLOCK] = part.astype(jnp.bfloat16)

    def own_slots(chunk):
        first = 0 if chunk else 1
        landed(row_slots.at[pl.ds(chunk * PER_CHUNK + first, PER_CHUNK - first)], own_slot_sem.at[chunk])

    def pass_slots(part):
        for source, sem, to in ((BELOW, BELOW_SLOTS, above), (ABOVE, ABOVE_SLOTS, below)):
            remote(
                slot_block(OWN, part), slot_block(source, part), send_sem.at[2], slot_sem.at[sem + part], to
            ).start()

    def ring_slots(part):
        for side, (source, sem, to) in enumerate(((BELOW, BELOW_SLOTS, above), (ABOVE, ABOVE_SLOTS, below))):
            landed(slot_block(source, part), slot_sem.at[sem + part])
            remote(
                slot_block(source, part, side), slot_block(ACROSS, part, side), send_sem.at[5],
                slot_sem.at[ACROSS_SLOTS + part], to,
            ).start()

    def across_slots(part):
        landed(slot_block(ACROSS, part), slot_sem.at[ACROSS_SLOTS + part])

    def pair(source, index):
        return [source + 2 * index, source + 2 * index + 1]

    def around(index):
        return pair(BELOW, index) + pair(ABOVE, index)

    def both(action, index):
        action(2 * index)
        action(2 * index + 1)

    def pick(step, *values):
        at = values[0]
        for k in range(1, len(values)):
            at = jnp.where(step == k, values[k], at)
        return at

    def early(step, _):
        @pl.when(step == 0)
        def _():
            with jax.named_scope("w0"):
                both(own_slots, 0)
                pass_slots(0)
                both(on_own, 0)
                widen(OWN)
                widen(OWN + 1)

        @pl.when(step == 1)
        def _():
            with jax.named_scope("w1"):
                for i in range(1, CHUNKS // 2):
                    both(own_slots, i)
                pass_slots(1)
                both(on_own, 1)
                widen(OWN + 2)
                widen(OWN + 3)

        @pl.when(step == 2)
        def _():
            with jax.named_scope("w2"):
                on_own(4)
                ring_slots(0)
                widen(BELOW)
                widen(ABOVE)
                on_ring(0)

        @pl.when(step == 3)
        def _():
            with jax.named_scope("w3"):
                on_ring(1)
                ring_slots(1)

        @pl.when(step == 4)
        def _():
            with jax.named_scope("w4"):
                on_ring(2)

        chunks = zip(pair(OWN, 0), pair(OWN, 1), (BELOW, ABOVE), (BELOW + 1, ABOVE + 1), (OWN + 4, BELOW + 2))
        later = zip(pair(OWN, 0) * 2, pair(OWN, 0) * 2, (BELOW + 1, ABOVE + 1) * 2, (OWN + 4, BELOW + 2) * 2, mixed)
        with jax.named_scope("early"):
            add([pick(step, *options) for options in chunks], [pick(step, *options) for options in later])
        return 0

    mixed = [OWN + 5, BELOW + 3, ABOVE + 2, ABOVE + 3]
    lax.fori_loop(0, 5, early, 0)

    last = CHUNKS // 2 - 1
    none = [0] * 4

    def late(step, _):
        @pl.when(step != 1)
        def _():
            @pl.when(step == 0)
            def _():
                with jax.named_scope("wr0"):
                    on_own(5)
                    on_ring(3)
                    on_own(6)
                    across_slots(0)

            @pl.when(step > 0)
            def _():
                with jax.named_scope("wr"):
                    @pl.when(step == 2)
                    def _():
                        both(on_ring, 2)
                        across_slots(1)

                    pl.when(step == 3)(functools.partial(on_ring, 7))

            chunks = zip(mixed, none, around(2), around(3))
            later = zip(pair(ACROSS, 0) * 2, none, pair(ACROSS, 1) * 2, pair(ACROSS, 2) * 2)
            with jax.named_scope("ring"):
                add([pick(step, *options) for options in chunks], [pick(step, *options) for options in later])

        @pl.when(step == 0)
        def _():
            with jax.named_scope("wa0"):
                both(on_across, 0)

        @pl.when(step == 1)
        def _():
            with jax.named_scope("wo"):
                on_own(7)

        @pl.when(step > 1)
        def _():
            with jax.named_scope("wa"):
                both(on_across, step - 1)
                pl.when(step == 2)(functools.partial(on_ring, 6))

        chunks = zip(pair(ACROSS, 0), pair(OWN, 3), pair(ACROSS, 1), pair(ACROSS, 2))
        later = zip(pair(OWN, 3) * 2, around(2), around(3), pair(ACROSS, 3) * 2)
        with jax.named_scope("single"):
            add([pick(step, *options) for options in chunks], [pick(step, *options) for options in later])
        return 0

    lax.fori_loop(0, 4, late, 0)
    with jax.named_scope("w_last"):
        both(on_across, last)
    with jax.named_scope("last"):
        add(pair(ACROSS, last), [])
        finish()

    def give_back(step, _):
        chunk = CHUNKS - 1 - step
        with jax.named_scope("gather"):
            wide = wide_of(chunk)
            offset = in_half(wide) - lanes(wide.shape)
            chosen = jnp.concatenate(
                [jnp.where(offset == i * BLOCK, 1.0, 0.0).astype(jnp.bfloat16) for i in range(HALF // BLOCK)], axis=1
            )
            sides = jnp.dot(chosen, mean[...], preferred_element_type=jnp.float32)
            picked = jnp.where(wide >= HALF, sides[:, BLOCK:], sides[:, :BLOCK])
            picked = jnp.where(wide >= 0, picked, 0.0)
            back[chunk] = picked.astype(jnp.bfloat16).reshape(PER_CHUNK, CAP, BLOCK)

        def send_back(chunk, place, to):
            remote(
                back.at[chunk, place], returned_out.at[0, me], send_sem.at[6], back_sem, {"grp": group, "mem": to}
            ).start()

        with jax.named_scope("sendback"):
            everyone(chunk, -1, send_back)

        return 0

    lax.fori_loop(0, CHUNKS, give_back, 0)
    returned_out[0, me] = back[0, 0]

    most = pl.ds(0, MEMBERS - 1)
    with jax.named_scope("lefts"):
        left(sent_slots.at[most], send_sem.at[0])
        left(values.at[0, most], send_sem.at[1])
        left(row_slots.at[pl.ds(0, 2 * MEMBERS)], send_sem.at[2])
        left(rows.at[pl.ds(0, 2 * CHUNKS + 1)], send_sem.at[3])
        left(rows.at[pl.ds(0, CHUNKS - 1)], send_sem.at[4])
        left(row_slots.at[pl.ds(0, MEMBERS)], send_sem.at[5])
        left(values.at[0, most], send_sem.at[6])
    with jax.named_scope("waitback"):
        landed(returned_out.at[0, most], back_sem)


PARTS = 8


def hand_over(averaged, returned, averaged_out, returned_out, sem):
    part = BUCKET // PARTS
    copies = [pltpu.make_async_copy(returned, returned_out, sem.at[PARTS])]
    for i in range(PARTS):
        at = pl.ds(i * part, part)
        copies.append(pltpu.make_async_copy(averaged.at[at], averaged_out.at[at], sem.at[i]))
    for copy in copies:
        copy.start()
    for copy in copies:
        copy.wait()


def per_device(values, slots, counts):
    in_hbm = pl.BlockSpec(memory_space=pltpu.HBM)
    in_vmem = pl.BlockSpec(memory_space=pltpu.VMEM)
    operands = [pltpu.with_memory_space_constraint(x, pltpu.HBM) for x in (values, jnp.swapaxes(slots, 1, 2), counts)]
    results = pl.pallas_call(
        kernel,
        out_shape=(
            jax.ShapeDtypeStruct((BUCKET, BLOCK), jnp.float32),
            jax.ShapeDtypeStruct((1, MEMBERS, CAP, BLOCK), jnp.bfloat16),
        ),
        in_specs=[in_hbm] * 3,
        out_specs=(in_vmem, in_vmem),
        scratch_shapes=[
            pltpu.VMEM((1, MEMBERS, CAP, BLOCK), jnp.bfloat16),
            pltpu.VMEM((1, CAP, MEMBERS), jnp.int32),
            pltpu.VMEM((1, MEMBERS), jnp.int32),
            pltpu.VMEM((MEMBERS, 1, BLOCK), jnp.int32),
            pltpu.VMEM((GROUPS * CHUNKS, PER_CHUNK, CAP, BLOCK), jnp.bfloat16),
            pltpu.VMEM((GROUPS * MEMBERS, 1, BLOCK), jnp.int32),
            pltpu.VMEM((GROUPS * MEMBERS, CAP, BLOCK), jnp.int32),
            pltpu.VMEM((HALF, 2 * BLOCK), jnp.float32),
            pltpu.VMEM((MEMBERS, BLOCK), jnp.float32),
            pltpu.VMEM((HALF, 2 * BLOCK), jnp.bfloat16),
            pltpu.VMEM((CHUNKS, PER_CHUNK, CAP, BLOCK), jnp.bfloat16),
            pltpu.SemaphoreType.DMA((3,)),
            pltpu.SemaphoreType.DMA((7,)),
            pltpu.SemaphoreType.DMA((CHUNKS,)),
            pltpu.SemaphoreType.DMA((3 * CHUNKS,)),
            pltpu.SemaphoreType.DMA((CHUNKS,)),
            pltpu.SemaphoreType.DMA((6,)),
            pltpu.SemaphoreType.DMA,
        ],
        compiler_params=pltpu.CompilerParams(
            collective_id=0, has_side_effects=True, vmem_limit_bytes=40 * 2**20
        ),
        name="merge",
    )(*operands)
    return pl.pallas_call(
        hand_over,
        out_shape=[jax.ShapeDtypeStruct(x.shape, x.dtype) for x in results],
        in_specs=[in_vmem, in_vmem],
        out_specs=[in_hbm, in_hbm],
        scratch_shapes=[pltpu.SemaphoreType.DMA((PARTS + 1,))],
        compiler_params=pltpu.CompilerParams(vmem_limit_bytes=2**20),
        name="hand_over",
    )(*results)


def solution(mesh):
    return jax.shard_map(
        per_device,
        mesh=mesh,
        in_specs=(
            P(("grp", "mem"), None, None, None),
            P(("grp", "mem"), None, None),
            P(("grp", "mem"), None),
        ),
        out_specs=(P("mem", None), P(("grp", "mem"), None, None, None)),
        check_vma=False,
    )
```

```python
import functools

import jax
import jax.numpy as jnp
from jax import lax
from jax.experimental import pallas as pl
from jax.experimental.pallas import tpu as pltpu
from jax.sharding import PartitionSpec as P

MESH = pl.DeviceIdType.MESH

GROUPS = 4
MEMBERS = 64
CAP = 32
BLOCK = 128
BUCKET = 7168
HALF = BUCKET // 2
PER_CHUNK = 8
CHUNKS = MEMBERS // PER_CHUNK
ROWS = PER_CHUNK * CAP
EARLY = 2 * PER_CHUNK

OWN, BELOW, ABOVE, ACROSS = 0, CHUNKS, 2 * CHUNKS, 3 * CHUNKS

BELOW_SLOTS, ABOVE_SLOTS, ACROSS_SLOTS = 0, 2, 4


def z_step(chunk):
    odd = lax.rem(chunk, 2)
    return odd * lax.div(chunk + 1, 2) + (1 - odd) * lax.rem(8 - lax.div(chunk, 2), 8)


def lanes(shape):
    return lax.broadcasted_iota(jnp.int32, shape, len(shape) - 1)


def in_half(slot):
    return jnp.where(slot >= HALF, slot - HALF, slot)


def kernel(
    values_in, slots_in, counts_in, averaged_out, returned_out,
    values, slots, counts, sent_slots, rows, row_slots, wide_slots, sums, tally, mean, back,
    load_sem, send_sem, own_sem, ring_sem, own_slot_sem, slot_sem, back_sem,
):
    group = lax.axis_index("grp")
    me = lax.axis_index("mem")
    above = {"grp": lax.rem(group + 1, GROUPS), "mem": me}
    below = {"grp": lax.rem(group + GROUPS - 1, GROUPS), "mem": me}
    across = {"grp": lax.rem(group + 2, GROUPS), "mem": me}
    z, x, core = lax.div(me, 8), lax.rem(lax.div(me, 2), 4), lax.rem(me, 2)
    def columns(sign):
        cores = [lax.rem(core + i, 2) for i in range(2)]
        return [2 * lax.rem(x + 4 + sign * i, 4) + cores[j] for i in range(4) for j in range(2)]

    def everyone(chunk, sign, reach):
        z_to = 8 * lax.rem(z + 8 + sign * z_step(chunk), 8)
        for place, column in enumerate(columns(sign)):
            if place:
                reach(chunk, place, z_to + column)
            else:
                pl.when(chunk > 0)(functools.partial(reach, chunk, place, z_to + column))

    def remote(source, target, send, recv, where):
        return pltpu.make_async_remote_copy(
            src_ref=source, dst_ref=target, send_sem=send, recv_sem=recv, device_id=where, device_id_type=MESH
        )

    def landed(ref, sem):
        remote(ref, ref, send_sem.at[0], sem, above).wait_recv()

    def left(ref, sem):
        remote(ref, ref, sem, back_sem, above).wait_send()

    barrier = pltpu.get_barrier_semaphore()

    def greet(chunk, place, to):
        pl.semaphore_signal(barrier, inc=1, device_id={"grp": group, "mem": to}, device_id_type=MESH)

    with jax.named_scope("greet"):
        lax.fori_loop(0, CHUNKS, lambda i, _: everyone(CHUNKS - 1 - i, 1, greet) or 0, 0)
        for other in (above, below, across):
            pl.semaphore_signal(barrier, inc=1, device_id=other, device_id_type=MESH)

    loads = [
        pltpu.make_async_copy(source, target, load_sem.at[i])
        for i, (source, target) in enumerate(((slots_in, slots), (counts_in, counts), (values_in, values)))
    ]
    for load in loads:
        load.start()

    with jax.named_scope("prep"):
        for load in loads[:2]:
            load.wait()
        is_valid = lax.broadcasted_iota(jnp.int32, (CAP, MEMBERS), 0) < counts[...]
        masked = jnp.where(is_valid, slots[0], -1)
        tiled = jnp.transpose(jnp.concatenate([masked] * 4, axis=0))
        sent_slots[...] = tiled.reshape(MEMBERS, 1, BLOCK)
        row_slots[0] = sent_slots[me]
        loads[2].wait()
        rows[0, 0] = values[0, me]
        sums[...] = jnp.zeros_like(sums)
        tally[...] = jnp.zeros_like(tally)

    with jax.named_scope("barrier"):
        pl.semaphore_wait(barrier, MEMBERS - 1 + GROUPS - 1)

    def send_slots(chunk, place, to):
        remote(
            sent_slots.at[to], row_slots.at[chunk * PER_CHUNK + place], send_sem.at[0], own_slot_sem.at[chunk],
            {"grp": group, "mem": to},
        ).start()

    def send_values(chunk, place, to):
        remote(
            values.at[0, to], rows.at[chunk, place], send_sem.at[1], own_sem.at[chunk], {"grp": group, "mem": to}
        ).start()

    with jax.named_scope("sends"):
        lax.fori_loop(0, CHUNKS, lambda i, _: everyone(i, 1, send_slots) or 0, 0)
        lax.fori_loop(0, CHUNKS, lambda i, _: everyone(i, 1, send_values) or 0, 0)

    def slot_block(source, part, side=None):
        first, count = (EARLY, MEMBERS - EARLY) if part else (0, EARLY)
        if side is not None:
            count = count // 2
            first = first + side * count
        return row_slots.at[pl.ds(source * PER_CHUNK + first, count)]

    def on_own(chunk):
        if isinstance(chunk, int) and chunk == 0:
            landed(rows.at[0, pl.ds(1, PER_CHUNK - 1)], own_sem.at[0])
        else:
            landed(rows.at[chunk], own_sem.at[chunk])
        remote(rows.at[chunk], rows.at[BELOW + chunk], send_sem.at[3], ring_sem.at[chunk], above).start()
        remote(rows.at[chunk], rows.at[ABOVE + chunk], send_sem.at[3], ring_sem.at[CHUNKS + chunk], below).start()
        if isinstance(chunk, int) and chunk == CHUNKS - 1:
            remote(
                rows.at[chunk], rows.at[ACROSS + chunk], send_sem.at[3], ring_sem.at[2 * CHUNKS + chunk], across
            ).start()

    some = PER_CHUNK // 2

    def on_ring(chunk):
        if isinstance(chunk, int) and chunk == CHUNKS - 1:
            landed(rows.at[BELOW + chunk], ring_sem.at[chunk])
            landed(rows.at[ABOVE + chunk], ring_sem.at[CHUNKS + chunk])
            return
        landed(rows.at[BELOW + chunk], ring_sem.at[chunk])
        first, last = pl.ds(0, some), pl.ds(some, some)
        remote(
            rows.at[BELOW + chunk, first], rows.at[ACROSS + chunk, first], send_sem.at[4],
            ring_sem.at[2 * CHUNKS + chunk], above,
        ).start()
        landed(rows.at[ABOVE + chunk], ring_sem.at[CHUNKS + chunk])
        remote(
            rows.at[ABOVE + chunk, last], rows.at[ACROSS + chunk, last], send_sem.at[4],
            ring_sem.at[2 * CHUNKS + chunk], below,
        ).start()

    def on_across(chunk):
        landed(rows.at[ACROSS + chunk], ring_sem.at[2 * CHUNKS + chunk])

    def widen(chunk):
        first = chunk * PER_CHUNK
        turned = jnp.transpose(row_slots[pl.ds(first, PER_CHUNK)].reshape(PER_CHUNK, BLOCK))
        for k in range(PER_CHUNK):
            wide_slots[first + k] = jnp.broadcast_to(turned[:CAP, k : k + 1], (CAP, BLOCK))

    def wide_of(chunk):
        return wide_slots[pl.ds(chunk * PER_CHUNK, PER_CHUNK)].reshape(ROWS, BLOCK)

    def lines_of(chunk):
        got = row_slots[pl.ds(chunk * PER_CHUNK, PER_CHUNK)].reshape(PER_CHUNK, BLOCK)
        quarter = lanes((1, BLOCK)) // CAP
        lines = []
        for q in range(0, PER_CHUNK, 4):
            line = got[q : q + 1]
            for i in range(1, 4):
                line = jnp.where(quarter == i, got[q + i : q + i + 1], line)
            lines.append(line)
        return lines

    def add(chunks, later):
        line = jnp.concatenate([line for chunk in chunks for line in lines_of(chunk)], axis=1)
        wide = jnp.concatenate([wide_of(chunk) for chunk in chunks], axis=0)
        over = line - lax.broadcasted_iota(jnp.int32, (MEMBERS, line.shape[1]), 0) * BLOCK
        by_block = jnp.where((over >= 0) & (over < BLOCK), 1.0, 0.0).astype(jnp.bfloat16)
        by_lane = jnp.where(lanes(wide.shape) == (wide & (BLOCK - 1)), 1.0, 0.0).astype(jnp.bfloat16)
        tally[...] += jnp.dot(by_block, by_lane, preferred_element_type=jnp.float32)
        got = jnp.concatenate([rows[chunk].reshape(ROWS, BLOCK) for chunk in chunks], axis=0).astype(jnp.float32)
        second = jnp.where(wide >= HALF, got, 0.0)
        right = jnp.concatenate([got - second, second], axis=1).astype(jnp.bfloat16)
        place = lax.broadcasted_iota(jnp.int32, (HALF, line.shape[1]), 0)
        chosen = jnp.where(place == in_half(line), 1.0, 0.0).astype(jnp.bfloat16)
        sums[...] += jnp.dot(chosen, right, preferred_element_type=jnp.float32)
        for chunk in later:
            widen(chunk)

    def finish():
        scale = jnp.transpose(1.0 / jnp.maximum(tally[...], 1.0))
        for j in range(HALF // BLOCK):
            at = j * BLOCK
            for side in range(2):
                column = side * (HALF // BLOCK) + j
                part = sums[at : at + BLOCK, side * BLOCK : (side + 1) * BLOCK]
                part = part * jnp.broadcast_to(scale[:, column : column + 1], (BLOCK, BLOCK))
                averaged_out[side * HALF + at : side * HALF + at + BLOCK, :] = part
                mean[at : at + BLOCK, side * BLOCK : (side + 1) * BLOCK] = part.astype(jnp.bfloat16)

    def own_slots(chunk):
        first = 0 if chunk else 1
        landed(row_slots.at[pl.ds(chunk * PER_CHUNK + first, PER_CHUNK - first)], own_slot_sem.at[chunk])

    def pass_slots(part):
        for source, sem, to in ((BELOW, BELOW_SLOTS, above), (ABOVE, ABOVE_SLOTS, below)):
            remote(
                slot_block(OWN, part), slot_block(source, part), send_sem.at[2], slot_sem.at[sem + part], to
            ).start()

    def ring_slots(part):
        for side, (source, sem, to) in enumerate(((BELOW, BELOW_SLOTS, above), (ABOVE, ABOVE_SLOTS, below))):
            landed(slot_block(source, part), slot_sem.at[sem + part])
            remote(
                slot_block(source, part, side), slot_block(ACROSS, part, side), send_sem.at[5],
                slot_sem.at[ACROSS_SLOTS + part], to,
            ).start()

    def across_slots(part):
        landed(slot_block(ACROSS, part), slot_sem.at[ACROSS_SLOTS + part])

    def pair(source, index):
        return [source + 2 * index, source + 2 * index + 1]

    def around(index):
        return pair(BELOW, index) + pair(ABOVE, index)

    def both(action, index):
        action(2 * index)
        action(2 * index + 1)

    def pick(step, *values):
        at = values[0]
        for k in range(1, len(values)):
            at = jnp.where(step == k, values[k], at)
        return at

    def early(step, _):
        @pl.when(step == 0)
        def _():
            with jax.named_scope("w0"):
                both(own_slots, 0)
                pass_slots(0)
                both(on_own, 0)
                widen(OWN)
                widen(OWN + 1)

        @pl.when(step == 1)
        def _():
            with jax.named_scope("w1"):
                for i in range(1, CHUNKS // 2):
                    both(own_slots, i)
                pass_slots(1)
                on_own(2)
                widen(OWN + 2)
            with jax.named_scope("one"):
                add([OWN + 2], [OWN + 3, OWN + 4])

        @pl.when(step == 2)
        def _():
            with jax.named_scope("w2"):
                on_own(3)
                ring_slots(0)
                widen(BELOW)
                widen(ABOVE)
                on_ring(0)

        @pl.when(step == 3)
        def _():
            with jax.named_scope("w3"):
                on_own(4)

        @pl.when(step == 4)
        def _():
            with jax.named_scope("w4"):
                on_ring(1)
                ring_slots(1)

        @pl.when(step == 5)
        def _():
            with jax.named_scope("w5"):
                on_ring(2)

        @pl.when(step != 1)
        def _():
            first, second, third = (BELOW, ABOVE), (BELOW + 1, ABOVE + 1), (BELOW + 2, ABOVE + 2)
            chunks = zip(pair(OWN, 0), (0, 0), first, (OWN + 3, OWN + 4), second, third)
            later = zip(pair(OWN, 0) * 2, none, second * 2, second * 2, third * 2, mixed)
            with jax.named_scope("early"):
                add([pick(step, *options) for options in chunks], [pick(step, *options) for options in later])

        return 0

    last = CHUNKS // 2 - 1
    none = [0] * 4
    mixed = [BELOW + 3, ABOVE + 3, OWN + 5, OWN + 6]
    lax.fori_loop(0, 6, early, 0)

    def late(step, _):
        @pl.when(step != 1)
        def _():
            @pl.when(step == 0)
            def _():
                with jax.named_scope("wr0"):
                    on_own(5)
                    on_ring(3)
                    on_own(6)
                    across_slots(0)

            @pl.when(step > 0)
            def _():
                with jax.named_scope("wr"):
                    @pl.when(step == 2)
                    def _():
                        both(on_ring, 2)
                        across_slots(1)

                    pl.when(step == 3)(functools.partial(on_ring, 7))

            chunks = zip(mixed, none, around(2), around(3))
            later = zip(pair(ACROSS, 0) + [OWN + 7] * 2, none, pair(ACROSS, 1) * 2, pair(ACROSS, 2) * 2)
            with jax.named_scope("ring"):
                add([pick(step, *options) for options in chunks], [pick(step, *options) for options in later])

            @pl.when(step == 0)
            def _():
                with jax.named_scope("wa0"):
                    both(on_across, 0)

            @pl.when(step > 0)
            def _():
                with jax.named_scope("wa"):
                    both(on_across, step - 1)
                    pl.when(step == 2)(functools.partial(on_ring, 6))

            chunks = zip(pair(ACROSS, 0), (0, 0), pair(ACROSS, 1), pair(ACROSS, 2))
            later = zip(around(2), none, around(3), pair(ACROSS, 3) * 2)
            with jax.named_scope("single"):
                add([pick(step, *options) for options in chunks], [pick(step, *options) for options in later])

        @pl.when(step == 1)
        def _():
            with jax.named_scope("wo"):
                on_own(7)
            with jax.named_scope("one"):
                add([OWN + 7], [])

        return 0

    lax.fori_loop(0, 4, late, 0)
    with jax.named_scope("w_last"):
        both(on_across, last)
    with jax.named_scope("last"):
        add(pair(ACROSS, last), [])
        finish()

    def give_back(step, _):
        chunk = CHUNKS - 1 - step
        with jax.named_scope("gather"):
            wide = wide_of(chunk)
            offset = in_half(wide) - lanes(wide.shape)
            chosen = jnp.concatenate(
                [jnp.where(offset == i * BLOCK, 1.0, 0.0).astype(jnp.bfloat16) for i in range(HALF // BLOCK)], axis=1
            )
            sides = jnp.dot(chosen, mean[...], preferred_element_type=jnp.float32)
            picked = jnp.where(wide >= HALF, sides[:, BLOCK:], sides[:, :BLOCK])
            picked = jnp.where(wide >= 0, picked, 0.0)
            back[chunk] = picked.astype(jnp.bfloat16).reshape(PER_CHUNK, CAP, BLOCK)

        def send_back(chunk, place, to):
            remote(
                back.at[chunk, place], returned_out.at[0, me], send_sem.at[6], back_sem, {"grp": group, "mem": to}
            ).start()

        with jax.named_scope("sendback"):
            everyone(chunk, -1, send_back)

        return 0

    lax.fori_loop(0, CHUNKS, give_back, 0)
    returned_out[0, me] = back[0, 0]

    most = pl.ds(0, MEMBERS - 1)
    with jax.named_scope("lefts"):
        left(sent_slots.at[most], send_sem.at[0])
        left(values.at[0, most], send_sem.at[1])
        left(row_slots.at[pl.ds(0, 2 * MEMBERS)], send_sem.at[2])
        left(rows.at[pl.ds(0, 2 * CHUNKS + 1)], send_sem.at[3])
        left(rows.at[pl.ds(0, CHUNKS - 1)], send_sem.at[4])
        left(row_slots.at[pl.ds(0, MEMBERS)], send_sem.at[5])
        left(values.at[0, most], send_sem.at[6])
    with jax.named_scope("waitback"):
        landed(returned_out.at[0, most], back_sem)


PARTS = 8


def hand_over(averaged, returned, averaged_out, returned_out, sem):
    part = BUCKET // PARTS
    copies = [pltpu.make_async_copy(returned, returned_out, sem.at[PARTS])]
    for i in range(PARTS):
        at = pl.ds(i * part, part)
        copies.append(pltpu.make_async_copy(averaged.at[at], averaged_out.at[at], sem.at[i]))
    for copy in copies:
        copy.start()
    for copy in copies:
        copy.wait()


def per_device(values, slots, counts):
    in_hbm = pl.BlockSpec(memory_space=pltpu.HBM)
    in_vmem = pl.BlockSpec(memory_space=pltpu.VMEM)
    operands = [pltpu.with_memory_space_constraint(x, pltpu.HBM) for x in (values, jnp.swapaxes(slots, 1, 2), counts)]
    results = pl.pallas_call(
        kernel,
        out_shape=(
            jax.ShapeDtypeStruct((BUCKET, BLOCK), jnp.float32),
            jax.ShapeDtypeStruct((1, MEMBERS, CAP, BLOCK), jnp.bfloat16),
        ),
        in_specs=[in_hbm] * 3,
        out_specs=(in_vmem, in_vmem),
        scratch_shapes=[
            pltpu.VMEM((1, MEMBERS, CAP, BLOCK), jnp.bfloat16),
            pltpu.VMEM((1, CAP, MEMBERS), jnp.int32),
            pltpu.VMEM((1, MEMBERS), jnp.int32),
            pltpu.VMEM((MEMBERS, 1, BLOCK), jnp.int32),
            pltpu.VMEM((GROUPS * CHUNKS, PER_CHUNK, CAP, BLOCK), jnp.bfloat16),
            pltpu.VMEM((GROUPS * MEMBERS, 1, BLOCK), jnp.int32),
            pltpu.VMEM((GROUPS * MEMBERS, CAP, BLOCK), jnp.int32),
            pltpu.VMEM((HALF, 2 * BLOCK), jnp.float32),
            pltpu.VMEM((MEMBERS, BLOCK), jnp.float32),
            pltpu.VMEM((HALF, 2 * BLOCK), jnp.bfloat16),
            pltpu.VMEM((CHUNKS, PER_CHUNK, CAP, BLOCK), jnp.bfloat16),
            pltpu.SemaphoreType.DMA((3,)),
            pltpu.SemaphoreType.DMA((7,)),
            pltpu.SemaphoreType.DMA((CHUNKS,)),
            pltpu.SemaphoreType.DMA((3 * CHUNKS,)),
            pltpu.SemaphoreType.DMA((CHUNKS,)),
            pltpu.SemaphoreType.DMA((6,)),
            pltpu.SemaphoreType.DMA,
        ],
        compiler_params=pltpu.CompilerParams(
            collective_id=0, has_side_effects=True, vmem_limit_bytes=40 * 2**20
        ),
        name="merge",
    )(*operands)
    return pl.pallas_call(
        hand_over,
        out_shape=[jax.ShapeDtypeStruct(x.shape, x.dtype) for x in results],
        in_specs=[in_vmem, in_vmem],
        out_specs=[in_hbm, in_hbm],
        scratch_shapes=[pltpu.SemaphoreType.DMA((PARTS + 1,))],
        compiler_params=pltpu.CompilerParams(vmem_limit_bytes=2**20),
        name="hand_over",
    )(*results)


def solution(mesh):
    return jax.shard_map(
        per_device,
        mesh=mesh,
        in_specs=(
            P(("grp", "mem"), None, None, None),
            P(("grp", "mem"), None, None),
            P(("grp", "mem"), None),
        ),
        out_specs=(P("mem", None), P(("grp", "mem"), None, None, None)),
        check_vma=False,
    )
```

```python
import functools

import jax
import jax.numpy as jnp
from jax import lax
from jax.experimental import pallas as pl
from jax.experimental.pallas import tpu as pltpu
from jax.sharding import PartitionSpec as P

MESH = pl.DeviceIdType.MESH

GROUPS = 4
MEMBERS = 64
CAP = 32
BLOCK = 128
BUCKET = 7168
HALF = BUCKET // 2
PER_CHUNK = 8
CHUNKS = MEMBERS // PER_CHUNK
ROWS = PER_CHUNK * CAP
EARLY = 2 * PER_CHUNK

OWN, BELOW, ABOVE, ACROSS = 0, CHUNKS, 2 * CHUNKS, 3 * CHUNKS

BELOW_SLOTS, ABOVE_SLOTS, ACROSS_SLOTS = 0, 2, 4


def z_step(chunk):
    odd = lax.rem(chunk, 2)
    return odd * lax.div(chunk + 1, 2) + (1 - odd) * lax.rem(8 - lax.div(chunk, 2), 8)


def lanes(shape):
    return lax.broadcasted_iota(jnp.int32, shape, len(shape) - 1)


def in_half(slot):
    return jnp.where(slot >= HALF, slot - HALF, slot)


def kernel(
    values_in, slots_in, counts_in, averaged_out, returned_out,
    values, slots, counts, sent_slots, rows, row_slots, wide_slots, sums, tally, mean, back,
    load_sem, send_sem, own_sem, ring_sem, own_slot_sem, slot_sem, back_sem,
):
    group = lax.axis_index("grp")
    me = lax.axis_index("mem")
    above = {"grp": lax.rem(group + 1, GROUPS), "mem": me}
    below = {"grp": lax.rem(group + GROUPS - 1, GROUPS), "mem": me}
    across = {"grp": lax.rem(group + 2, GROUPS), "mem": me}
    z, x, core = lax.div(me, 8), lax.rem(lax.div(me, 2), 4), lax.rem(me, 2)
    def columns(sign):
        cores = [lax.rem(core + i, 2) for i in range(2)]
        return [2 * lax.rem(x + 4 + sign * i, 4) + cores[j] for i in range(4) for j in range(2)]

    def everyone(chunk, sign, reach):
        z_to = 8 * lax.rem(z + 8 + sign * z_step(chunk), 8)
        for place, column in enumerate(columns(sign)):
            if place:
                reach(chunk, place, z_to + column)
            else:
                pl.when(chunk > 0)(functools.partial(reach, chunk, place, z_to + column))

    def remote(source, target, send, recv, where):
        return pltpu.make_async_remote_copy(
            src_ref=source, dst_ref=target, send_sem=send, recv_sem=recv, device_id=where, device_id_type=MESH
        )

    def landed(ref, sem):
        remote(ref, ref, send_sem.at[0], sem, above).wait_recv()

    def left(ref, sem):
        remote(ref, ref, sem, back_sem, above).wait_send()

    barrier = pltpu.get_barrier_semaphore()

    def greet(chunk, place, to):
        pl.semaphore_signal(barrier, inc=1, device_id={"grp": group, "mem": to}, device_id_type=MESH)

    with jax.named_scope("greet"):
        lax.fori_loop(0, CHUNKS, lambda i, _: everyone(CHUNKS - 1 - i, 1, greet) or 0, 0)
        for other in (above, below, across):
            pl.semaphore_signal(barrier, inc=1, device_id=other, device_id_type=MESH)

    loads = [
        pltpu.make_async_copy(source, target, load_sem.at[i])
        for i, (source, target) in enumerate(((slots_in, slots), (counts_in, counts), (values_in, values)))
    ]
    for load in loads:
        load.start()

    with jax.named_scope("prep"):
        for load in loads[:2]:
            load.wait()
        is_valid = lax.broadcasted_iota(jnp.int32, (CAP, MEMBERS), 0) < counts[...]
        masked = jnp.where(is_valid, slots[0], -1)
        tiled = jnp.transpose(jnp.concatenate([masked] * 4, axis=0))
        sent_slots[...] = tiled.reshape(MEMBERS, 1, BLOCK)
        row_slots[0] = sent_slots[me]
        loads[2].wait()
        rows[0, 0] = values[0, me]
        sums[...] = jnp.zeros_like(sums)
        tally[...] = jnp.zeros_like(tally)

    with jax.named_scope("barrier"):
        pl.semaphore_wait(barrier, MEMBERS - 1 + GROUPS - 1)

    def send_slots(chunk, place, to):
        remote(
            sent_slots.at[to], row_slots.at[chunk * PER_CHUNK + place], send_sem.at[0], own_slot_sem.at[chunk],
            {"grp": group, "mem": to},
        ).start()

    def send_values(chunk, place, to):
        remote(
            values.at[0, to], rows.at[chunk, place], send_sem.at[1], own_sem.at[chunk], {"grp": group, "mem": to}
        ).start()

    with jax.named_scope("sends"):
        lax.fori_loop(0, CHUNKS, lambda i, _: everyone(i, 1, send_slots) or 0, 0)
        lax.fori_loop(0, CHUNKS, lambda i, _: everyone(i, 1, send_values) or 0, 0)

    def slot_block(source, part, side=None):
        first, count = (EARLY, MEMBERS - EARLY) if part else (0, EARLY)
        if side is not None:
            count = count // 2
            first = first + side * count
        return row_slots.at[pl.ds(source * PER_CHUNK + first, count)]

    def on_own(chunk):
        if isinstance(chunk, int) and chunk == 0:
            landed(rows.at[0, pl.ds(1, PER_CHUNK - 1)], own_sem.at[0])
        else:
            landed(rows.at[chunk], own_sem.at[chunk])
        remote(rows.at[chunk], rows.at[BELOW + chunk], send_sem.at[3], ring_sem.at[chunk], above).start()
        remote(rows.at[chunk], rows.at[ABOVE + chunk], send_sem.at[3], ring_sem.at[CHUNKS + chunk], below).start()
        if isinstance(chunk, int) and chunk == CHUNKS - 1:
            remote(
                rows.at[chunk], rows.at[ACROSS + chunk], send_sem.at[3], ring_sem.at[2 * CHUNKS + chunk], across
            ).start()

    some = PER_CHUNK // 2

    def on_ring(chunk):
        if isinstance(chunk, int) and chunk == CHUNKS - 1:
            landed(rows.at[BELOW + chunk], ring_sem.at[chunk])
            landed(rows.at[ABOVE + chunk], ring_sem.at[CHUNKS + chunk])
            return
        landed(rows.at[BELOW + chunk], ring_sem.at[chunk])
        first, last = pl.ds(0, some), pl.ds(some, some)
        remote(
            rows.at[BELOW + chunk, first], rows.at[ACROSS + chunk, first], send_sem.at[4],
            ring_sem.at[2 * CHUNKS + chunk], above,
        ).start()
        landed(rows.at[ABOVE + chunk], ring_sem.at[CHUNKS + chunk])
        remote(
            rows.at[ABOVE + chunk, last], rows.at[ACROSS + chunk, last], send_sem.at[4],
            ring_sem.at[2 * CHUNKS + chunk], below,
        ).start()

    def on_across(chunk):
        landed(rows.at[ACROSS + chunk], ring_sem.at[2 * CHUNKS + chunk])

    def widen(chunk):
        first = chunk * PER_CHUNK
        turned = jnp.transpose(row_slots[pl.ds(first, PER_CHUNK)].reshape(PER_CHUNK, BLOCK))
        for k in range(PER_CHUNK):
            wide_slots[first + k] = jnp.broadcast_to(turned[:CAP, k : k + 1], (CAP, BLOCK))

    def wide_of(chunk):
        return wide_slots[pl.ds(chunk * PER_CHUNK, PER_CHUNK)].reshape(ROWS, BLOCK)

    def lines_of(chunk):
        got = row_slots[pl.ds(chunk * PER_CHUNK, PER_CHUNK)].reshape(PER_CHUNK, BLOCK)
        quarter = lanes((1, BLOCK)) // CAP
        lines = []
        for q in range(0, PER_CHUNK, 4):
            line = got[q : q + 1]
            for i in range(1, 4):
                line = jnp.where(quarter == i, got[q + i : q + i + 1], line)
            lines.append(line)
        return lines

    def add(chunks, later):
        line = jnp.concatenate([line for chunk in chunks for line in lines_of(chunk)], axis=1)
        wide = jnp.concatenate([wide_of(chunk) for chunk in chunks], axis=0)
        over = line - lax.broadcasted_iota(jnp.int32, (MEMBERS, line.shape[1]), 0) * BLOCK
        by_block = jnp.where((over >= 0) & (over < BLOCK), 1.0, 0.0).astype(jnp.bfloat16)
        by_lane = jnp.where(lanes(wide.shape) == (wide & (BLOCK - 1)), 1.0, 0.0).astype(jnp.bfloat16)
        tally[...] += jnp.dot(by_block, by_lane, preferred_element_type=jnp.float32)
        got = jnp.concatenate([rows[chunk].reshape(ROWS, BLOCK) for chunk in chunks], axis=0).astype(jnp.float32)
        second = jnp.where(wide >= HALF, got, 0.0)
        right = jnp.concatenate([got - second, second], axis=1).astype(jnp.bfloat16)
        place = lax.broadcasted_iota(jnp.int32, (HALF, line.shape[1]), 0)
        chosen = jnp.where(place == in_half(line), 1.0, 0.0).astype(jnp.bfloat16)
        sums[...] += jnp.dot(chosen, right, preferred_element_type=jnp.float32)
        for chunk in later:
            widen(chunk)

    def finish():
        scale = jnp.transpose(1.0 / jnp.maximum(tally[...], 1.0))
        for j in range(HALF // BLOCK):
            at = j * BLOCK
            for side in range(2):
                column = side * (HALF // BLOCK) + j
                part = sums[at : at + BLOCK, side * BLOCK : (side + 1) * BLOCK]
                part = part * jnp.broadcast_to(scale[:, column : column + 1], (BLOCK, BLOCK))
                averaged_out[side * HALF + at : side * HALF + at + BLOCK, :] = part
                mean[at : at + BLOCK, side * BLOCK : (side + 1) * BLOCK] = part.astype(jnp.bfloat16)

    def own_slots(chunk):
        first = 0 if chunk else 1
        landed(row_slots.at[pl.ds(chunk * PER_CHUNK + first, PER_CHUNK - first)], own_slot_sem.at[chunk])

    def pass_slots(part):
        for source, sem, to in ((BELOW, BELOW_SLOTS, above), (ABOVE, ABOVE_SLOTS, below)):
            remote(
                slot_block(OWN, part), slot_block(source, part), send_sem.at[2], slot_sem.at[sem + part], to
            ).start()

    def ring_slots(part):
        for side, (source, sem, to) in enumerate(((BELOW, BELOW_SLOTS, above), (ABOVE, ABOVE_SLOTS, below))):
            landed(slot_block(source, part), slot_sem.at[sem + part])
            remote(
                slot_block(source, part, side), slot_block(ACROSS, part, side), send_sem.at[5],
                slot_sem.at[ACROSS_SLOTS + part], to,
            ).start()

    def across_slots(part):
        landed(slot_block(ACROSS, part), slot_sem.at[ACROSS_SLOTS + part])

    def pair(source, index):
        return [source + 2 * index, source + 2 * index + 1]

    def around(index):
        return pair(BELOW, index) + pair(ABOVE, index)

    def both(action, index):
        action(2 * index)
        action(2 * index + 1)

    def pick(step, *values):
        at = values[0]
        for k in range(1, len(values)):
            at = jnp.where(step == k, values[k], at)
        return at

    def early(step, _):
        @pl.when(step == 0)
        def _():
            with jax.named_scope("w0"):
                both(own_slots, 0)
                pass_slots(0)
                both(on_own, 0)
                widen(OWN)
                widen(OWN + 1)

        @pl.when(step == 1)
        def _():
            with jax.named_scope("w1"):
                for i in range(1, CHUNKS // 2):
                    both(own_slots, i)
                pass_slots(1)
                on_own(2)
                widen(OWN + 2)
            with jax.named_scope("one"):
                add([OWN + 2], [OWN + 3, OWN + 4])

        @pl.when(step == 2)
        def _():
            with jax.named_scope("w2"):
                on_own(3)
                ring_slots(0)
                widen(BELOW)
                widen(ABOVE)
                on_ring(0)

        @pl.when(step == 3)
        def _():
            with jax.named_scope("w3"):
                on_own(4)

        @pl.when(step == 4)
        def _():
            with jax.named_scope("w4"):
                on_ring(1)
                ring_slots(1)

        @pl.when(step == 5)
        def _():
            with jax.named_scope("w5"):
                on_ring(2)

        @pl.when(step != 1)
        def _():
            first, second, third = (BELOW, ABOVE), (BELOW + 1, ABOVE + 1), (BELOW + 2, ABOVE + 2)
            chunks = zip(pair(OWN, 0), (0, 0), first, (OWN + 3, OWN + 4), second, third)
            later = zip(pair(OWN, 0) * 2, none, second * 2, second * 2, third * 2, mixed)
            with jax.named_scope("early"):
                add([pick(step, *options) for options in chunks], [pick(step, *options) for options in later])

        return 0

    last = CHUNKS // 2 - 1
    none = [0] * 4
    mixed = [BELOW + 3, ABOVE + 3, OWN + 5, OWN + 6]
    lax.fori_loop(0, 6, early, 0)

    def late(step, _):
        @pl.when(step != 1)
        def _():
            @pl.when(step == 0)
            def _():
                with jax.named_scope("wr0"):
                    on_own(5)
                    on_ring(3)
                    on_own(6)
                    across_slots(0)

            @pl.when(step > 0)
            def _():
                with jax.named_scope("wr"):
                    @pl.when(step == 2)
                    def _():
                        both(on_ring, 2)
                        across_slots(1)

                    pl.when(step == 3)(functools.partial(on_ring, 7))

            chunks = zip(mixed, none, around(2), around(3))
            later = zip(pair(ACROSS, 0) + [OWN + 7] * 2, none, pair(ACROSS, 1) * 2, pair(ACROSS, 2) * 2)
            with jax.named_scope("ring"):
                add([pick(step, *options) for options in chunks], [pick(step, *options) for options in later])

            @pl.when(step == 0)
            def _():
                with jax.named_scope("wa0"):
                    both(on_across, 0)

            @pl.when(step > 0)
            def _():
                with jax.named_scope("wa"):
                    both(on_across, step - 1)
                    pl.when(step == 2)(functools.partial(on_ring, 6))

            chunks = zip(pair(ACROSS, 0), (0, 0), pair(ACROSS, 1), pair(ACROSS, 2))
            later = zip(around(2), none, around(3), pair(ACROSS, 3) * 2)
            with jax.named_scope("single"):
                add([pick(step, *options) for options in chunks], [pick(step, *options) for options in later])

        @pl.when(step == 1)
        def _():
            with jax.named_scope("wo"):
                on_own(7)
            with jax.named_scope("one"):
                add([OWN + 7], [])

        return 0

    lax.fori_loop(0, 4, late, 0)
    with jax.named_scope("w_last"):
        both(on_across, last)
    with jax.named_scope("last"):
        add(pair(ACROSS, last), [])
        finish()

    def give_back(step, _):
        chunk = CHUNKS - 1 - step
        with jax.named_scope("gather"):
            wide = wide_of(chunk)
            offset = in_half(wide) - lanes(wide.shape)
            chosen = jnp.concatenate(
                [jnp.where(offset == i * BLOCK, 1.0, 0.0).astype(jnp.bfloat16) for i in range(HALF // BLOCK)], axis=1
            )
            sides = jnp.dot(chosen, mean[...], preferred_element_type=jnp.float32)
            picked = jnp.where(wide >= HALF, sides[:, BLOCK:], sides[:, :BLOCK])
            back[chunk] = picked.astype(jnp.bfloat16).reshape(PER_CHUNK, CAP, BLOCK)

        def send_back(chunk, place, to):
            remote(
                back.at[chunk, place], returned_out.at[0, me], send_sem.at[6], back_sem, {"grp": group, "mem": to}
            ).start()

        with jax.named_scope("sendback"):
            everyone(chunk, -1, send_back)

        return 0

    lax.fori_loop(0, CHUNKS, give_back, 0)
    returned_out[0, me] = back[0, 0]

    most = pl.ds(0, MEMBERS - 1)
    with jax.named_scope("lefts"):
        left(sent_slots.at[most], send_sem.at[0])
        left(values.at[0, most], send_sem.at[1])
        left(row_slots.at[pl.ds(0, 2 * MEMBERS)], send_sem.at[2])
        left(rows.at[pl.ds(0, 2 * CHUNKS + 1)], send_sem.at[3])
        left(rows.at[pl.ds(0, CHUNKS - 1)], send_sem.at[4])
        left(row_slots.at[pl.ds(0, MEMBERS)], send_sem.at[5])
        left(values.at[0, most], send_sem.at[6])
    with jax.named_scope("waitback"):
        landed(returned_out.at[0, most], back_sem)


PARTS = 8


def hand_over(averaged, returned, averaged_out, returned_out, sem):
    part = BUCKET // PARTS
    copies = [pltpu.make_async_copy(returned, returned_out, sem.at[PARTS])]
    for i in range(PARTS):
        at = pl.ds(i * part, part)
        copies.append(pltpu.make_async_copy(averaged.at[at], averaged_out.at[at], sem.at[i]))
    for copy in copies:
        copy.start()
    for copy in copies:
        copy.wait()


def per_device(values, slots, counts):
    in_hbm = pl.BlockSpec(memory_space=pltpu.HBM)
    in_vmem = pl.BlockSpec(memory_space=pltpu.VMEM)
    operands = [pltpu.with_memory_space_constraint(x, pltpu.HBM) for x in (values, jnp.swapaxes(slots, 1, 2), counts)]
    results = pl.pallas_call(
        kernel,
        out_shape=(
            jax.ShapeDtypeStruct((BUCKET, BLOCK), jnp.float32),
            jax.ShapeDtypeStruct((1, MEMBERS, CAP, BLOCK), jnp.bfloat16),
        ),
        in_specs=[in_hbm] * 3,
        out_specs=(in_vmem, in_vmem),
        scratch_shapes=[
            pltpu.VMEM((1, MEMBERS, CAP, BLOCK), jnp.bfloat16),
            pltpu.VMEM((1, CAP, MEMBERS), jnp.int32),
            pltpu.VMEM((1, MEMBERS), jnp.int32),
            pltpu.VMEM((MEMBERS, 1, BLOCK), jnp.int32),
            pltpu.VMEM((GROUPS * CHUNKS, PER_CHUNK, CAP, BLOCK), jnp.bfloat16),
            pltpu.VMEM((GROUPS * MEMBERS, 1, BLOCK), jnp.int32),
            pltpu.VMEM((GROUPS * MEMBERS, CAP, BLOCK), jnp.int32),
            pltpu.VMEM((HALF, 2 * BLOCK), jnp.float32),
            pltpu.VMEM((MEMBERS, BLOCK), jnp.float32),
            pltpu.VMEM((HALF, 2 * BLOCK), jnp.bfloat16),
            pltpu.VMEM((CHUNKS, PER_CHUNK, CAP, BLOCK), jnp.bfloat16),
            pltpu.SemaphoreType.DMA((3,)),
            pltpu.SemaphoreType.DMA((7,)),
            pltpu.SemaphoreType.DMA((CHUNKS,)),
            pltpu.SemaphoreType.DMA((3 * CHUNKS,)),
            pltpu.SemaphoreType.DMA((CHUNKS,)),
            pltpu.SemaphoreType.DMA((6,)),
            pltpu.SemaphoreType.DMA,
        ],
        compiler_params=pltpu.CompilerParams(
            collective_id=0, has_side_effects=True, vmem_limit_bytes=40 * 2**20,
        ),
        name="merge",
    )(*operands)
    return pl.pallas_call(
        hand_over,
        out_shape=[jax.ShapeDtypeStruct(x.shape, x.dtype) for x in results],
        in_specs=[in_vmem, in_vmem],
        out_specs=[in_hbm, in_hbm],
        scratch_shapes=[pltpu.SemaphoreType.DMA((PARTS + 1,))],
        compiler_params=pltpu.CompilerParams(vmem_limit_bytes=2**20),
        name="hand_over",
    )(*results)


def solution(mesh):
    return jax.shard_map(
        per_device,
        mesh=mesh,
        in_specs=(
            P(("grp", "mem"), None, None, None),
            P(("grp", "mem"), None, None),
            P(("grp", "mem"), None),
        ),
        out_specs=(P("mem", None), P(("grp", "mem"), None, None, None)),
        check_vma=False,
    )
```

```python
import functools

import jax
import jax.numpy as jnp
from jax import lax
from jax.experimental import pallas as pl
from jax.experimental.pallas import tpu as pltpu
from jax.sharding import PartitionSpec as P

MESH = pl.DeviceIdType.MESH

GROUPS = 4
MEMBERS = 64
CAP = 32
BLOCK = 128
BUCKET = 7168
HALF = BUCKET // 2
PER_CHUNK = 8
CHUNKS = MEMBERS // PER_CHUNK
ROWS = PER_CHUNK * CAP
EARLY = 2 * PER_CHUNK

OWN, BELOW, ABOVE, ACROSS = 0, CHUNKS, 2 * CHUNKS, 3 * CHUNKS

BELOW_SLOTS, ABOVE_SLOTS, ACROSS_SLOTS = 0, 2, 4


def z_step(chunk):
    odd = lax.rem(chunk, 2)
    return odd * lax.div(chunk + 1, 2) + (1 - odd) * lax.rem(8 - lax.div(chunk, 2), 8)


def lanes(shape):
    return lax.broadcasted_iota(jnp.int32, shape, len(shape) - 1)


def in_half(slot):
    return jnp.where(slot >= HALF, slot - HALF, slot)


def kernel(
    values_in, slots_in, counts_in, averaged_out, returned_out,
    values, slots, counts, sent_slots, rows, row_slots, wide_slots, sums, tally, mean, back,
    load_sem, send_sem, own_sem, ring_sem, own_slot_sem, slot_sem, back_sem,
):
    group = lax.axis_index("grp")
    me = lax.axis_index("mem")
    above = {"grp": lax.rem(group + 1, GROUPS), "mem": me}
    below = {"grp": lax.rem(group + GROUPS - 1, GROUPS), "mem": me}
    across = {"grp": lax.rem(group + 2, GROUPS), "mem": me}
    z, x, core = lax.div(me, 8), lax.rem(lax.div(me, 2), 4), lax.rem(me, 2)
    def columns(sign):
        cores = [lax.rem(core + i, 2) for i in range(2)]
        return [2 * lax.rem(x + 4 + sign * i, 4) + cores[j] for i in range(4) for j in range(2)]

    def everyone(chunk, sign, reach):
        z_to = 8 * lax.rem(z + 8 + sign * z_step(chunk), 8)
        for place, column in enumerate(columns(sign)):
            if place:
                reach(chunk, place, z_to + column)
            else:
                pl.when(chunk > 0)(functools.partial(reach, chunk, place, z_to + column))

    def remote(source, target, send, recv, where):
        return pltpu.make_async_remote_copy(
            src_ref=source, dst_ref=target, send_sem=send, recv_sem=recv, device_id=where, device_id_type=MESH
        )

    def landed(ref, sem):
        remote(ref, ref, send_sem.at[0], sem, above).wait_recv()

    def left(ref, sem):
        remote(ref, ref, sem, back_sem, above).wait_send()

    barrier = pltpu.get_barrier_semaphore()

    def greet(chunk, place, to):
        pl.semaphore_signal(barrier, inc=1, device_id={"grp": group, "mem": to}, device_id_type=MESH)

    with jax.named_scope("greet"):
        lax.fori_loop(0, CHUNKS, lambda i, _: everyone(CHUNKS - 1 - i, 1, greet) or 0, 0)
        for other in (above, below, across):
            pl.semaphore_signal(barrier, inc=1, device_id=other, device_id_type=MESH)

    loads = [
        pltpu.make_async_copy(source, target, load_sem.at[i])
        for i, (source, target) in enumerate(((slots_in, slots), (counts_in, counts), (values_in, values)))
    ]
    for load in loads:
        load.start()

    with jax.named_scope("prep"):
        for load in loads[:2]:
            load.wait()
        is_valid = lax.broadcasted_iota(jnp.int32, (CAP, MEMBERS), 0) < counts[...]
        masked = jnp.where(is_valid, slots[0], -1)
        tiled = jnp.transpose(jnp.concatenate([masked] * 4, axis=0))
        sent_slots[...] = tiled.reshape(MEMBERS, 1, BLOCK)
        row_slots[0] = sent_slots[me]
        loads[2].wait()
        rows[0, 0] = values[0, me]
        sums[...] = jnp.zeros_like(sums)
        tally[...] = jnp.zeros_like(tally)

    with jax.named_scope("barrier"):
        pl.semaphore_wait(barrier, MEMBERS - 1 + GROUPS - 1)

    def send_slots(chunk, place, to):
        remote(
            sent_slots.at[to], row_slots.at[chunk * PER_CHUNK + place], send_sem.at[0], own_slot_sem.at[chunk],
            {"grp": group, "mem": to},
        ).start()

    def send_values(chunk, place, to):
        remote(
            values.at[0, to], rows.at[chunk, place], send_sem.at[1], own_sem.at[chunk], {"grp": group, "mem": to}
        ).start()

    with jax.named_scope("sends"):
        lax.fori_loop(0, CHUNKS, lambda i, _: everyone(i, 1, send_slots) or 0, 0)
        lax.fori_loop(0, CHUNKS, lambda i, _: everyone(i, 1, send_values) or 0, 0)

    def slot_block(source, part, side=None):
        first, count = (EARLY, MEMBERS - EARLY) if part else (0, EARLY)
        if side is not None:
            count = count // 2
            first = first + side * count
        return row_slots.at[pl.ds(source * PER_CHUNK + first, count)]

    def on_own(chunk):
        if isinstance(chunk, int) and chunk == 0:
            landed(rows.at[0, pl.ds(1, PER_CHUNK - 1)], own_sem.at[0])
        else:
            landed(rows.at[chunk], own_sem.at[chunk])
        remote(rows.at[chunk], rows.at[BELOW + chunk], send_sem.at[3], ring_sem.at[chunk], above).start()
        remote(rows.at[chunk], rows.at[ABOVE + chunk], send_sem.at[3], ring_sem.at[CHUNKS + chunk], below).start()
        if isinstance(chunk, int) and chunk == CHUNKS - 1:
            remote(
                rows.at[chunk], rows.at[ACROSS + chunk], send_sem.at[3], ring_sem.at[2 * CHUNKS + chunk], across
            ).start()

    some = PER_CHUNK // 2

    def on_ring(chunk):
        if isinstance(chunk, int) and chunk == CHUNKS - 1:
            landed(rows.at[BELOW + chunk], ring_sem.at[chunk])
            landed(rows.at[ABOVE + chunk], ring_sem.at[CHUNKS + chunk])
            return
        landed(rows.at[BELOW + chunk], ring_sem.at[chunk])
        first, last = pl.ds(0, some), pl.ds(some, some)
        remote(
            rows.at[BELOW + chunk, first], rows.at[ACROSS + chunk, first], send_sem.at[4],
            ring_sem.at[2 * CHUNKS + chunk], above,
        ).start()
        landed(rows.at[ABOVE + chunk], ring_sem.at[CHUNKS + chunk])
        remote(
            rows.at[ABOVE + chunk, last], rows.at[ACROSS + chunk, last], send_sem.at[4],
            ring_sem.at[2 * CHUNKS + chunk], below,
        ).start()

    def on_across(chunk):
        landed(rows.at[ACROSS + chunk], ring_sem.at[2 * CHUNKS + chunk])

    def widen(chunk):
        first = chunk * PER_CHUNK
        turned = jnp.transpose(row_slots[pl.ds(first, PER_CHUNK)].reshape(PER_CHUNK, BLOCK))
        for k in range(PER_CHUNK):
            wide_slots[first + k] = jnp.broadcast_to(turned[:CAP, k : k + 1], (CAP, BLOCK))

    def wide_of(chunk):
        return wide_slots[pl.ds(chunk * PER_CHUNK, PER_CHUNK)].reshape(ROWS, BLOCK)

    def lines_of(chunk):
        got = row_slots[pl.ds(chunk * PER_CHUNK, PER_CHUNK)].reshape(PER_CHUNK, BLOCK)
        quarter = lanes((1, BLOCK)) // CAP
        lines = []
        for q in range(0, PER_CHUNK, 4):
            line = got[q : q + 1]
            for i in range(1, 4):
                line = jnp.where(quarter == i, got[q + i : q + i + 1], line)
            lines.append(line)
        return lines

    def add(chunks, later):
        line = jnp.concatenate([line for chunk in chunks for line in lines_of(chunk)], axis=1)
        wide = jnp.concatenate([wide_of(chunk) for chunk in chunks], axis=0)
        over = line - lax.broadcasted_iota(jnp.int32, (MEMBERS, line.shape[1]), 0) * BLOCK
        by_block = jnp.where((over >= 0) & (over < BLOCK), 1.0, 0.0).astype(jnp.bfloat16)
        by_lane = jnp.where(lanes(wide.shape) == (wide & (BLOCK - 1)), 1.0, 0.0).astype(jnp.bfloat16)
        tally[...] += jnp.dot(by_block, by_lane, preferred_element_type=jnp.float32)
        got = jnp.concatenate([rows[chunk].reshape(ROWS, BLOCK) for chunk in chunks], axis=0).astype(jnp.float32)
        second = jnp.where(wide >= HALF, got, 0.0)
        right = jnp.concatenate([got - second, second], axis=1).astype(jnp.bfloat16)
        place = lax.broadcasted_iota(jnp.int32, (HALF, line.shape[1]), 0)
        chosen = jnp.where(place == in_half(line), 1.0, 0.0).astype(jnp.bfloat16)
        sums[...] += jnp.dot(chosen, right, preferred_element_type=jnp.float32)
        for chunk in later:
            widen(chunk)

    def finish():
        scale = jnp.transpose(1.0 / jnp.maximum(tally[...], 1.0))
        for j in range(HALF // BLOCK):
            at = j * BLOCK
            for side in range(2):
                column = side * (HALF // BLOCK) + j
                part = sums[at : at + BLOCK, side * BLOCK : (side + 1) * BLOCK]
                part = part * jnp.broadcast_to(scale[:, column : column + 1], (BLOCK, BLOCK))
                averaged_out[side * HALF + at : side * HALF + at + BLOCK, :] = part
                mean[at : at + BLOCK, side * BLOCK : (side + 1) * BLOCK] = part.astype(jnp.bfloat16)

    def own_slots(chunk):
        first = 0 if chunk else 1
        landed(row_slots.at[pl.ds(chunk * PER_CHUNK + first, PER_CHUNK - first)], own_slot_sem.at[chunk])

    def pass_slots(part):
        for source, sem, to in ((BELOW, BELOW_SLOTS, above), (ABOVE, ABOVE_SLOTS, below)):
            remote(
                slot_block(OWN, part), slot_block(source, part), send_sem.at[2], slot_sem.at[sem + part], to
            ).start()

    def ring_slots(part):
        for side, (source, sem, to) in enumerate(((BELOW, BELOW_SLOTS, above), (ABOVE, ABOVE_SLOTS, below))):
            landed(slot_block(source, part), slot_sem.at[sem + part])
            remote(
                slot_block(source, part, side), slot_block(ACROSS, part, side), send_sem.at[5],
                slot_sem.at[ACROSS_SLOTS + part], to,
            ).start()

    def across_slots(part):
        landed(slot_block(ACROSS, part), slot_sem.at[ACROSS_SLOTS + part])

    def pair(source, index):
        return [source + 2 * index, source + 2 * index + 1]

    def around(index):
        return pair(BELOW, index) + pair(ABOVE, index)

    def both(action, index):
        action(2 * index)
        action(2 * index + 1)

    def pick(step, *values):
        at = values[0]
        for k in range(1, len(values)):
            at = jnp.where(step == k, values[k], at)
        return at

    def early(step, _):
        @pl.when(step == 0)
        def _():
            with jax.named_scope("w0"):
                both(own_slots, 0)
                pass_slots(0)
                both(on_own, 0)
                widen(OWN)
                widen(OWN + 1)

        @pl.when(step == 1)
        def _():
            with jax.named_scope("w1"):
                for i in range(1, CHUNKS // 2):
                    both(own_slots, i)
                pass_slots(1)
                on_own(2)
                widen(OWN + 2)
            with jax.named_scope("one"):
                add([OWN + 2], [OWN + 3, OWN + 4])

        @pl.when(step == 2)
        def _():
            with jax.named_scope("w2"):
                on_own(3)
                ring_slots(0)
                widen(BELOW)
                widen(ABOVE)
                on_ring(0)

        @pl.when(step == 3)
        def _():
            with jax.named_scope("w3"):
                on_own(4)

        @pl.when(step == 4)
        def _():
            with jax.named_scope("w4"):
                on_ring(1)
                ring_slots(1)

        @pl.when(step == 5)
        def _():
            with jax.named_scope("w5"):
                on_ring(2)

        @pl.when(step != 1)
        def _():
            first, second, third = (BELOW, ABOVE), (BELOW + 1, ABOVE + 1), (BELOW + 2, ABOVE + 2)
            chunks = zip(pair(OWN, 0), (0, 0), first, (OWN + 3, OWN + 4), second, third)
            later = zip(pair(OWN, 0) * 2, none, second * 2, second * 2, third * 2, mixed)
            with jax.named_scope("early"):
                add([pick(step, *options) for options in chunks], [pick(step, *options) for options in later])

        return 0

    last = CHUNKS // 2 - 1
    none = [0] * 4
    mixed = [BELOW + 3, ABOVE + 3, OWN + 5, OWN + 6]
    lax.fori_loop(0, 6, early, 0)

    def late(step, _):
        @pl.when(step != 1)
        def _():
            @pl.when(step == 0)
            def _():
                with jax.named_scope("wr0"):
                    on_own(5)
                    on_ring(3)
                    on_own(6)
                    across_slots(0)

            @pl.when(step > 0)
            def _():
                with jax.named_scope("wr"):
                    @pl.when(step == 2)
                    def _():
                        on_ring(5)
                        across_slots(1)

                    pl.when(step == 3)(functools.partial(on_ring, 7))

            chunks = zip(mixed, none, around(2), around(3))
            later = zip(pair(ACROSS, 0) + [OWN + 7] * 2, none, pair(ACROSS, 1) * 2, pair(ACROSS, 2) * 2)
            with jax.named_scope("ring"):
                add([pick(step, *options) for options in chunks], [pick(step, *options) for options in later])

            @pl.when(step == 0)
            def _():
                with jax.named_scope("wa0"):
                    both(on_across, 0)

            @pl.when(step > 0)
            def _():
                with jax.named_scope("wa"):
                    both(on_across, step - 1)
                    pl.when(step == 2)(functools.partial(on_ring, 6))

            chunks = zip(pair(ACROSS, 0), (0, 0), pair(ACROSS, 1), pair(ACROSS, 2))
            later = zip(around(2), none, around(3), pair(ACROSS, 3) * 2)
            with jax.named_scope("single"):
                add([pick(step, *options) for options in chunks], [pick(step, *options) for options in later])

        @pl.when(step == 1)
        def _():
            with jax.named_scope("wo"):
                on_ring(4)
                on_own(7)
            with jax.named_scope("one"):
                add([OWN + 7], [])

        return 0

    lax.fori_loop(0, 4, late, 0)
    with jax.named_scope("w_last"):
        both(on_across, last)
    with jax.named_scope("last"):
        add(pair(ACROSS, last), [])
        finish()

    def give_back(step, _):
        chunk = CHUNKS - 1 - step
        with jax.named_scope("gather"):
            wide = wide_of(chunk)
            offset = in_half(wide) - lanes(wide.shape)
            chosen = jnp.concatenate(
                [jnp.where(offset == i * BLOCK, 1.0, 0.0).astype(jnp.bfloat16) for i in range(HALF // BLOCK)], axis=1
            )
            sides = jnp.dot(chosen, mean[...], preferred_element_type=jnp.float32)
            picked = jnp.where(wide >= HALF, sides[:, BLOCK:], sides[:, :BLOCK])
            picked = jnp.where(wide >= 0, picked, 0.0)
            back[chunk] = picked.astype(jnp.bfloat16).reshape(PER_CHUNK, CAP, BLOCK)

        def send_back(chunk, place, to):
            remote(
                back.at[chunk, place], returned_out.at[0, me], send_sem.at[6], back_sem, {"grp": group, "mem": to}
            ).start()

        with jax.named_scope("sendback"):
            everyone(chunk, -1, send_back)

        return 0

    lax.fori_loop(0, CHUNKS, give_back, 0)
    returned_out[0, me] = back[0, 0]

    most = pl.ds(0, MEMBERS - 1)
    with jax.named_scope("lefts"):
        left(sent_slots.at[most], send_sem.at[0])
        left(values.at[0, most], send_sem.at[1])
        left(row_slots.at[pl.ds(0, 2 * MEMBERS)], send_sem.at[2])
        left(rows.at[pl.ds(0, 2 * CHUNKS + 1)], send_sem.at[3])
        left(rows.at[pl.ds(0, CHUNKS - 1)], send_sem.at[4])
        left(row_slots.at[pl.ds(0, MEMBERS)], send_sem.at[5])
        left(values.at[0, most], send_sem.at[6])
    with jax.named_scope("waitback"):
        landed(returned_out.at[0, most], back_sem)


PARTS = 8


def hand_over(averaged, returned, averaged_out, returned_out, sem):
    part = BUCKET // PARTS
    copies = [pltpu.make_async_copy(returned, returned_out, sem.at[PARTS])]
    for i in range(PARTS):
        at = pl.ds(i * part, part)
        copies.append(pltpu.make_async_copy(averaged.at[at], averaged_out.at[at], sem.at[i]))
    for copy in copies:
        copy.start()
    for copy in copies:
        copy.wait()


def per_device(values, slots, counts):
    in_hbm = pl.BlockSpec(memory_space=pltpu.HBM)
    in_vmem = pl.BlockSpec(memory_space=pltpu.VMEM)
    operands = [pltpu.with_memory_space_constraint(x, pltpu.HBM) for x in (values, jnp.swapaxes(slots, 1, 2), counts)]
    results = pl.pallas_call(
        kernel,
        out_shape=(
            jax.ShapeDtypeStruct((BUCKET, BLOCK), jnp.float32),
            jax.ShapeDtypeStruct((1, MEMBERS, CAP, BLOCK), jnp.bfloat16),
        ),
        in_specs=[in_hbm] * 3,
        out_specs=(in_vmem, in_vmem),
        scratch_shapes=[
            pltpu.VMEM((1, MEMBERS, CAP, BLOCK), jnp.bfloat16),
            pltpu.VMEM((1, CAP, MEMBERS), jnp.int32),
            pltpu.VMEM((1, MEMBERS), jnp.int32),
            pltpu.VMEM((MEMBERS, 1, BLOCK), jnp.int32),
            pltpu.VMEM((GROUPS * CHUNKS, PER_CHUNK, CAP, BLOCK), jnp.bfloat16),
            pltpu.VMEM((GROUPS * MEMBERS, 1, BLOCK), jnp.int32),
            pltpu.VMEM((GROUPS * MEMBERS, CAP, BLOCK), jnp.int32),
            pltpu.VMEM((HALF, 2 * BLOCK), jnp.float32),
            pltpu.VMEM((MEMBERS, BLOCK), jnp.float32),
            pltpu.VMEM((HALF, 2 * BLOCK), jnp.bfloat16),
            pltpu.VMEM((CHUNKS, PER_CHUNK, CAP, BLOCK), jnp.bfloat16),
            pltpu.SemaphoreType.DMA((3,)),
            pltpu.SemaphoreType.DMA((7,)),
            pltpu.SemaphoreType.DMA((CHUNKS,)),
            pltpu.SemaphoreType.DMA((3 * CHUNKS,)),
            pltpu.SemaphoreType.DMA((CHUNKS,)),
            pltpu.SemaphoreType.DMA((6,)),
            pltpu.SemaphoreType.DMA,
        ],
        compiler_params=pltpu.CompilerParams(
            collective_id=0, has_side_effects=True, vmem_limit_bytes=40 * 2**20
        ),
        name="merge",
    )(*operands)
    return pl.pallas_call(
        hand_over,
        out_shape=[jax.ShapeDtypeStruct(x.shape, x.dtype) for x in results],
        in_specs=[in_vmem, in_vmem],
        out_specs=[in_hbm, in_hbm],
        scratch_shapes=[pltpu.SemaphoreType.DMA((PARTS + 1,))],
        compiler_params=pltpu.CompilerParams(vmem_limit_bytes=2**20),
        name="hand_over",
    )(*results)


def solution(mesh):
    return jax.shard_map(
        per_device,
        mesh=mesh,
        in_specs=(
            P(("grp", "mem"), None, None, None),
            P(("grp", "mem"), None, None),
            P(("grp", "mem"), None),
        ),
        out_specs=(P("mem", None), P(("grp", "mem"), None, None, None)),
        check_vma=False,
    )
```
